256 devices in a mesh: dp: 32 (over x, y, core), tensor: 8 (over z).
Axes of the slice: x: 4, y: 4, z: 8, core: 2. Of those that a mesh axis runs over, the one named last changes fastest.
Arguments:
- query: bfloat16 [512, 4096], P('dp', 'tensor'), may hold values from -8000 to 8000
- incoming_key: bfloat16 [512, 2048], P('dp', 'tensor'), may hold values from -4.5 to 4.5
- new_value: bfloat16 [512, 2048], P('dp', 'tensor'), may hold values from -4.5 to 4.5
- key_cache: bfloat16 [512, 256, 2048], P('dp', None, 'tensor'), may hold values from -4.5 to 4.5
- value_cache: bfloat16 [512, 256, 2048], P('dp', None, 'tensor'), may hold values from -4.5 to 4.5
- cache_len: int32 [512], P('dp'), may hold values from 2 to 256
- out_weight: bfloat16 [4096, 4608], P('tensor'), may hold values from -0.09375 to 0.09375
- residual: bfloat16 [512, 4608], P('dp'), may hold values from -6 to 6
- post_gain: float32 [4608], replicated, may hold values from 0.5 to 1.5
- final_gain: float32 [4608], replicated, may hold values from 0.5 to 1.5
- vocab_weight: bfloat16 [131072, 4608], P(('dp', 'tensor')), may hold values from -113 to 113
- sampled: int32 [512], P('dp'), may hold values from 0 to 131071
- stop_flag: int32 [512], P('dp'), may hold values from 0 to 1, as said below
Outputs:
- new_residual: bfloat16 [512, 4608], P('dp', 'tensor')
- token_logprob: float32 [512], P('dp')
- insert_rank: int32 [512], P('dp')
- released_slot_total: int32 [], replicated
The draws below stay inside these ranges and needn't reach their ends.
Inputs may be any that keep to these rules, and one draw needn't show every extreme that they name: `stop_flag`: each aligned block of 16 slots holds 1 to 16 stops.
All inputs are finite; a program needn't handle non-finite values.
Results may differ from the reference program's by a relative error of at most 0.0038.
The reference program's roundings to bfloat16 on the way (of `weight`, `attn` and `hidden`) count: a program that leaves them out, or rounds other values in their place, can miss the bound.
Values may be sent and summed in bfloat16 or wider, within the bound.
No kernel may reach another device: no remote copies, remote signals or barrier semaphores. Data moves between devices by JAX's collectives and lax.ppermute only.
A program may use at most 64 MiB of HBM per device.

```python
import jax
import jax.numpy as jnp
from jax import lax

D = 4608
HEADS = 32
KV_HEADS = 16
HEAD_DIM = 128
VOCAB = 131072
SLOT_DEV = 16
CACHE = 256
SLOTS = 512


def joint_cache(key):
    first, second, third = jax.random.split(jax.random.fold_in(key, 7), 3)
    cache = jax.random.truncated_normal(first, -4.5, 4.5, (SLOTS, CACHE, KV_HEADS * HEAD_DIM), jnp.float32)
    query = jax.random.truncated_normal(second, -4.5, 4.5, (SLOTS, HEADS * HEAD_DIM), jnp.float32)
    group = HEADS // KV_HEADS
    target = jnp.exp(jax.random.uniform(third, (SLOTS,), jnp.float32, jnp.log(110.0), jnp.log(420.0)))
    chosen = jnp.arange(SLOTS) % 8 == 3
    lead = cache[:, 0].reshape(SLOTS, KV_HEADS, HEAD_DIM)
    norms = jnp.sum(lead * lead, axis=-1)
    strength = target[:, None] * 12.0 / norms
    scaled = strength[:, :, None] * lead
    aligned = jnp.broadcast_to(scaled[:, :, None, :], (SLOTS, KV_HEADS, group, HEAD_DIM)).reshape(SLOTS, HEADS * HEAD_DIM)
    query = jnp.where(chosen[:, None], aligned, query)
    factor = 1.0 - 2.0 / (target[:, None] + 4.0)
    nearby = (lead * factor[:, :, None]).reshape(SLOTS, KV_HEADS * HEAD_DIM)
    cache = cache.at[:, 1].set(jnp.where(chosen[:, None], nearby, cache[:, 1]))
    return (cache, query)


def draw_key_cache(key, part):
    cache, query = joint_cache(key)
    return cache.astype(jnp.bfloat16)


def draw_query(key, part):
    cache, query = joint_cache(key)
    return jnp.clip(query, -8000.0, 8000.0).astype(jnp.bfloat16)


def draw_vocab_weight(key, part):
    first, second, third = jax.random.split(jax.random.fold_in(key, 11), 3)
    weight = 0.05 * jax.random.truncated_normal(first, -6.0, 6.0, (VOCAB, D), jnp.float32)
    strong = jax.random.randint(second, (VOCAB,), 0, 32) == 0
    level = jnp.exp(jax.random.uniform(third, (VOCAB,), jnp.float32, jnp.log(40.0), jnp.log(100.0)))
    factor = level / (0.05 * jnp.sqrt(jnp.float32(D)))
    weight = jnp.where(strong[:, None], weight * factor[:, None], weight)
    return jnp.clip(weight, -113.0, 113.0).astype(jnp.bfloat16)


def draw_stop_flag(key, part):
    first, second = jax.random.split(jax.random.fold_in(key, 13))
    blocks = SLOTS // SLOT_DEV
    index = jnp.arange(blocks, dtype=jnp.int32)
    rising = 1 + (SLOT_DEV - 1) * index // max(blocks - 1, 1)
    jitter = jax.random.randint(first, (blocks,), 0, 2)
    counts = jnp.maximum(rising - jitter, 1)
    block_keys = jax.random.split(second, blocks)
    orders = jax.vmap(lambda k: jax.random.permutation(k, SLOT_DEV))(block_keys)
    return (orders < counts[:, None]).astype(jnp.int32).reshape(SLOTS)


def place_ends(entries, own_key, low, largest):
    spot = [jax.random.randint(jax.random.fold_in(own_key, axis), (), 0, length) for axis, length in enumerate(entries.shape)]
    longest = entries.shape.index(max(entries.shape))
    next_to = spot[:longest] + [(spot[longest] + 1) % entries.shape[longest]] + spot[longest + 1:]
    return entries.at[tuple(spot)].set(low).at[tuple(next_to)].set(largest)


def steps_of(stream_key, dims, cuts, least, top_value):
    def one(position, blocks):
        steps = jax.random.uniform(jax.random.fold_in(jax.random.fold_in(stream_key, 6), position), (blocks,), jnp.float32, least / len(cuts), top_value / len(cuts))
        return jnp.repeat(jnp.exp(steps), dims[position] // blocks).reshape((-1,) + (1,) * (len(dims) - position - 1))

    gain = one(*cuts[0])
    for cut in cuts[1:]:
        gain = gain * one(*cut)
    return gain


def gaussian(rng, shape, spread, reach, cuts=(), kind=jnp.bfloat16):
    result = spread * jax.random.normal(rng, shape, jnp.float32)
    if cuts:
        result = result * steps_of(rng, shape, cuts, -0.22, 0.18)
    return jnp.clip(result, -reach, reach).astype(kind)


def setup_inputs(seed: int = 0) -> dict:
    seeds = jax.random.split(jax.random.key(seed), 14)
    query = draw_query(jax.random.fold_in(seeds[13], 71), 0)
    incoming_key = gaussian(seeds[1], (SLOTS, KV_HEADS * HEAD_DIM), 1.0, 4.5, ((0, 32), (1, 8)))
    new_value = gaussian(seeds[2], (SLOTS, KV_HEADS * HEAD_DIM), 1.0, 4.5, ((0, 32), (1, 8)))
    key_cache = draw_key_cache(jax.random.fold_in(seeds[13], 71), 0)
    value_cache = gaussian(seeds[4], (SLOTS, CACHE, KV_HEADS * HEAD_DIM), 1.0, 4.5, ((0, 32), (2, 8)))
    cache_len = place_ends(jax.random.randint(seeds[5], (SLOTS,), 2, CACHE + 1), jax.random.fold_in(seeds[5], 1), 2, CACHE).astype(jnp.int32)
    out_weight = gaussian(seeds[6], (HEADS * HEAD_DIM, D), (HEADS * HEAD_DIM) ** -0.5, 0.09375, ((0, 8),))
    residual = gaussian(seeds[7], (SLOTS, D), 1.0, 6.0, ((0, 32),))
    post_gain = jnp.clip(1.0 + 0.1 * jax.random.normal(seeds[8], (D,), jnp.float32), 0.5, 1.5)
    final_gain = jnp.clip(1.0 + 0.1 * jax.random.normal(seeds[9], (D,), jnp.float32), 0.5, 1.5)
    vocab_weight = draw_vocab_weight(jax.random.fold_in(seeds[13], 71), 0)
    sampled = place_ends(jax.random.randint(seeds[11], (SLOTS,), 0, VOCAB), jax.random.fold_in(seeds[11], 1), 0, VOCAB - 1).astype(jnp.int32)
    stop_flag = draw_stop_flag(jax.random.fold_in(seeds[13], 71), 0)
    return {"query": query, "incoming_key": incoming_key, "new_value": new_value, "key_cache": key_cache, "value_cache": value_cache, "cache_len": cache_len, "out_weight": out_weight, "residual": residual, "post_gain": post_gain, "final_gain": final_gain, "vocab_weight": vocab_weight, "sampled": sampled, "stop_flag": stop_flag}


def attend_slot(items):
    query, incoming_key, new_value, key_cache, value_cache, length = items
    group = HEADS // KV_HEADS
    query_vector = query.astype(jnp.float32).reshape(KV_HEADS, group, HEAD_DIM)
    keys = key_cache.astype(jnp.float32).reshape(CACHE, KV_HEADS, HEAD_DIM)
    values = value_cache.astype(jnp.float32).reshape(CACHE, KV_HEADS, HEAD_DIM)
    self_key = incoming_key.astype(jnp.float32).reshape(KV_HEADS, HEAD_DIM)
    own_value = new_value.astype(jnp.float32).reshape(KV_HEADS, HEAD_DIM)
    scores = jnp.einsum('kgd,ckd->kgc', query_vector, keys) / 12.0
    self_entry = jnp.einsum('kgd,kd->kg', query_vector, self_key) / 12.0
    valid = jnp.arange(CACHE, dtype=jnp.int32)[None, None, :] < length
    scores = jnp.where(valid, scores, -1e+30)
    top = jnp.maximum(lax.optimization_barrier(jnp.max(scores, axis=-1)), self_entry)
    expo = jnp.where(valid, jnp.exp(scores - top[..., None]), 0.0)
    own_exp = jnp.exp(self_entry - top)
    total = lax.optimization_barrier(jnp.sum(expo, axis=-1)) + own_exp
    weight = (expo / total[..., None]).astype(jnp.bfloat16).astype(jnp.float32)
    own_weight = (own_exp / total).astype(jnp.bfloat16).astype(jnp.float32)
    attn = jnp.einsum('kgc,ckd->kgd', weight, values) + own_weight[..., None] * own_value[:, None, :]
    return attn.reshape(HEADS * HEAD_DIM).astype(jnp.bfloat16)

def reference(query, incoming_key, new_value, key_cache, value_cache, cache_len, out_weight, residual, post_gain, final_gain, vocab_weight, sampled, stop_flag):
    attn = lax.map(attend_slot, (query, incoming_key, new_value, key_cache, value_cache, cache_len))
    proj = jnp.dot(attn, out_weight, preferred_element_type=jnp.float32)
    post = proj * lax.rsqrt(lax.optimization_barrier(jnp.mean(proj * proj, axis=1, keepdims=True)) + 1e-06) * post_gain
    new_residual = (residual.astype(jnp.float32) + post).astype(jnp.bfloat16)
    mixed = new_residual.astype(jnp.float32)
    hidden = (mixed * lax.rsqrt(lax.optimization_barrier(jnp.mean(mixed * mixed, axis=1, keepdims=True)) + 1e-06) * final_gain).astype(jnp.bfloat16)
    logits = lax.dot_general(hidden, vocab_weight, (((1,), (1,)), ((), ())), preferred_element_type=jnp.float32)
    top = lax.optimization_barrier(jnp.max(logits, axis=1))
    total = jnp.log(lax.optimization_barrier(jnp.sum(jnp.exp(logits - top[:, None]), axis=1))) + top
    picked = jnp.take_along_axis(logits, sampled[:, None].astype(jnp.int32), axis=1)[:, 0]
    token_logprob = picked - total
    freed = (stop_flag == 1).astype(jnp.int32)
    before = (jnp.cumsum(freed) - freed).astype(jnp.int32)
    insert_rank = jnp.where(freed == 1, before, -1).astype(jnp.int32)
    released_slot_total = jnp.sum(freed).astype(jnp.int32)
    return (new_residual, token_logprob, insert_rank, released_slot_total)
```

```python
import jax
import jax.numpy as jnp
from jax import lax
from jax.sharding import Mesh
from jax.sharding import PartitionSpec as P

D = 4608
HEADS = 32
KV_HEADS = 16
HEAD_DIM = 128
DP = ("dp_0", "dp_1", "dp_2")
DP_TENSOR = ("dp_0", "dp_1", "dp_2", "tensor")
PLANE = ("dp_0", "dp_1")
CHIPS = ("dp_0", "dp_1", "tensor")
META = 128


def attend_local(query, incoming_key, new_value, key_cache, value_cache, cache_len):
    slot_dev = query.shape[0]
    positions = key_cache.shape[1]
    kv_local = incoming_key.shape[1] // HEAD_DIM
    group = HEADS // KV_HEADS
    query_vector = query.reshape(slot_dev, kv_local, group, HEAD_DIM)
    keys = key_cache.reshape(slot_dev, positions, kv_local, HEAD_DIM)
    values = value_cache.reshape(slot_dev, positions, kv_local, HEAD_DIM)
    self_key = incoming_key.reshape(slot_dev, kv_local, HEAD_DIM)
    own_value = new_value.reshape(slot_dev, kv_local, HEAD_DIM).astype(jnp.float32)
    scores = (
        jnp.einsum("bkgd,bckd->bkgc", query_vector, keys, preferred_element_type=jnp.float32) / 12.0
    )
    self_entry = (
        jnp.einsum("qyxm,qym->qyx", query_vector, self_key, preferred_element_type=jnp.float32)
        / 12.0
    )
    valid = (
        jnp.arange(positions, dtype=jnp.int32)[None, None, None, :] < cache_len[:, None, None, None]
    )
    scores = jnp.where(valid, scores, -1e30)
    top = jnp.maximum(jnp.max(scores, axis=-1), self_entry)
    expo = jnp.where(valid, jnp.exp(scores - top[..., None]), 0.0)
    own_exp = jnp.exp(self_entry - top)
    total = jnp.sum(expo, axis=-1) + own_exp
    weight = (expo / total[..., None]).astype(jnp.bfloat16)
    own_weight = (own_exp / total).astype(jnp.bfloat16).astype(jnp.float32)
    attn = jnp.einsum("bkgc,bckd->bkgd", weight, values, preferred_element_type=jnp.float32)
    attn = attn + own_weight[..., None] * own_value[:, :, None, :]
    return attn.astype(jnp.bfloat16).reshape(slot_dev, kv_local * group * HEAD_DIM)


def exchange(blocks, axes):
    return lax.all_to_all(blocks, axes, 0, 0, tiled=True)


def spread(block, axes):
    count = 1
    for axis in axes if isinstance(axes, tuple) else (axes,):
        count *= lax.axis_size(axis)
    return exchange(jnp.broadcast_to(block[None], (count, *block.shape)), axes)


def other_core(value):
    return lax.ppermute(value, "dp_2", [(0, 1), (1, 0)])


def inverse_rms(rows):
    return lax.rsqrt(jnp.mean(rows * rows, axis=-1, keepdims=True) + 1e-06)


def vocab_part(every, ids, rows, start):
    logits = lax.dot_general(
        every, rows, (((1,), (1,)), ((), ())), preferred_element_type=jnp.float32
    )
    hit = jnp.arange(rows.shape[0], dtype=jnp.int32)[None, :] == (ids - start)[:, None]
    picked = jnp.sum(jnp.where(hit, logits, 0.0), axis=1)
    top = jnp.max(logits, axis=1)
    total = jnp.sum(jnp.exp(logits - top[:, None]), axis=1)
    return top, total, picked


def on_device(
    query,
    incoming_key,
    new_value,
    key_cache,
    value_cache,
    cache_len,
    out_weight,
    residual,
    post_gain,
    final_gain,
    vocab_weight,
    sampled,
    stop_flag,
):
    slot_dev = query.shape[0]
    nz = lax.axis_size("tensor")
    z = lax.axis_index("tensor")
    core = lax.axis_index("dp_2")
    plane = lax.axis_index(PLANE)
    planes = lax.axis_size(PLANE)
    freed = (stop_flag == 1).astype(jnp.int32)
    count = jnp.sum(freed)

    vocab_other = other_core(vocab_weight)
    count_other = other_core(jnp.broadcast_to(count.astype(jnp.float32), (8, 128)))[0, 0]

    attn = attend_local(query, incoming_key, new_value, key_cache, value_cache, cache_len)
    partial_value = jnp.dot(attn, out_weight, preferred_element_type=jnp.float32)
    per = slot_dev // nz
    pieces = exchange(partial_value.astype(jnp.bfloat16).reshape(nz, per, D), "tensor")
    proj = jnp.sum(pieces.astype(jnp.float32), axis=0)
    post = proj * inverse_rms(proj) * post_gain
    own_residual = lax.dynamic_slice_in_dim(residual, z * per, per, 0)
    mix = (own_residual.astype(jnp.float32) + post).astype(jnp.bfloat16)
    full_mix = spread(mix, "tensor").reshape(slot_dev, D)
    mixed = full_mix.astype(jnp.float32)
    hidden = (mixed * inverse_rms(mixed) * final_gain).astype(jnp.bfloat16)
    width = D // nz
    new_residual = lax.dynamic_slice_in_dim(full_mix, z * width, width, 1)

    meta = jnp.stack(
        [
            sampled & 63,
            (sampled >> 6) & 63,
            sampled >> 12,
            freed,
            jnp.broadcast_to(count_other.astype(jnp.int32), (slot_dev,)),
        ],
        axis=1,
    ).astype(jnp.bfloat16)
    meta = jnp.pad(meta, ((0, 0), (0, META - meta.shape[1])))
    every = spread(jnp.concatenate([hidden, meta], axis=1), PLANE)
    every = every.reshape(planes * slot_dev, D + META)
    notes = every[:, D : D + 5].astype(jnp.int32)
    ids = notes[:, 0] + notes[:, 1] * 64 + notes[:, 2] * 4096
    every = every[:, :D]

    per_device = vocab_weight.shape[0]
    start = (lax.axis_index(DP) * nz + z) * per_device
    start_other = ((plane * 2 + 1 - core) * nz + z) * per_device
    top_a, sum_a, picked_a = vocab_part(every, ids, vocab_weight, start)
    top_b, sum_b, picked_b = vocab_part(every, ids, vocab_other, start_other)
    top = jnp.maximum(top_a, top_b)
    total = sum_a * jnp.exp(top_a - top) + sum_b * jnp.exp(top_b - top)
    pair = jnp.stack([top + jnp.log(total), picked_a + picked_b], axis=0)
    pair = pair.reshape(2, planes, slot_dev).transpose(1, 0, 2).reshape(planes, 1, 2 * slot_dev)
    pair = jnp.broadcast_to(pair, (planes, nz, 2 * slot_dev)).reshape(planes * nz, 2 * slot_dev)
    gathered = exchange(pair, CHIPS)
    parts = gathered[:, :slot_dev]
    highest = jnp.max(parts, axis=0)
    overall = jnp.log(jnp.sum(jnp.exp(parts - highest[None]), axis=0)) + highest
    token_logprob = jnp.sum(gathered[:, slot_dev:], axis=0) - overall

    flags = notes[:, 3].reshape(planes, slot_dev)
    counts_here = jnp.sum(flags, axis=1)
    counts_there = notes[:, 4].reshape(planes, slot_dev)[:, 0]
    chips = jnp.arange(planes, dtype=jnp.int32)
    both = counts_here + counts_there
    before = jnp.sum(jnp.where(chips < plane, both, 0))
    before = before + jnp.where(core == 1, count_other.astype(jnp.int32), 0)
    released = jnp.sum(both).astype(jnp.int32)
    insert_rank = jnp.where(freed == 1, jnp.cumsum(freed) - freed + before, -1)
    return (new_residual, token_logprob, insert_rank.astype(jnp.int32), released)


def solution(mesh):
    split = Mesh(
        mesh.devices.reshape(4, 4, 2, mesh.shape["tensor"]), ("dp_0", "dp_1", "dp_2", "tensor")
    )
    in_specs = (
        P(DP, "tensor"),
        P(DP, "tensor"),
        P(DP, "tensor"),
        P(DP, None, "tensor"),
        P(DP, None, "tensor"),
        P(DP),
        P("tensor", None),
        P(DP, None),
        P(),
        P(),
        P(DP_TENSOR, None),
        P(DP),
        P(DP),
    )
    out_specs = (P(DP, "tensor"), P(DP), P(DP), P())
    return jax.shard_map(
        on_device, mesh=split, in_specs=in_specs, out_specs=out_specs, check_vma=False
    )
```

```python
import jax
import jax.numpy as jnp
from jax import lax
from jax.experimental import pallas as pl
from jax.experimental.pallas import tpu as pltpu
from jax.sharding import Mesh
from jax.sharding import PartitionSpec as P

D = 4608
HEADS = 32
KV_HEADS = 16
HEAD_DIM = 128
DP = ("dp_0", "dp_1", "dp_2")
DP_TENSOR = ("dp_0", "dp_1", "dp_2", "tensor")
PLANE = ("dp_0", "dp_1")
CHIPS = ("dp_0", "dp_1", "tensor")
META = 128
TILE = 256
VMEM_GRANT = 60 * 1024 * 1024
LAST_GRANT = 60 * 1024 * 1024


def attend_local(query, incoming_key, new_value, key_cache, value_cache, cache_len):
    slot_dev = query.shape[0]
    positions = key_cache.shape[1]
    kv_local = incoming_key.shape[1] // HEAD_DIM
    group = HEADS // KV_HEADS
    query_vector = query.reshape(slot_dev, kv_local, group, HEAD_DIM)
    keys = key_cache.reshape(slot_dev, positions, kv_local, HEAD_DIM)
    values = value_cache.reshape(slot_dev, positions, kv_local, HEAD_DIM)
    self_key = incoming_key.reshape(slot_dev, kv_local, HEAD_DIM)
    own_value = new_value.reshape(slot_dev, kv_local, HEAD_DIM).astype(jnp.float32)
    scores = (
        jnp.einsum("bkgd,bckd->bkgc", query_vector, keys, preferred_element_type=jnp.float32) / 12.0
    )
    self_entry = (
        jnp.einsum("qyxm,qym->qyx", query_vector, self_key, preferred_element_type=jnp.float32)
        / 12.0
    )
    valid = (
        jnp.arange(positions, dtype=jnp.int32)[None, None, None, :] < cache_len[:, None, None, None]
    )
    scores = jnp.where(valid, scores, -1e30)
    top = jnp.maximum(jnp.max(scores, axis=-1), self_entry)
    expo = jnp.where(valid, jnp.exp(scores - top[..., None]), 0.0)
    own_exp = jnp.exp(self_entry - top)
    total = jnp.sum(expo, axis=-1) + own_exp
    weight = (expo / total[..., None]).astype(jnp.bfloat16)
    own_weight = (own_exp / total).astype(jnp.bfloat16).astype(jnp.float32)
    attn = jnp.einsum("bkgc,bckd->bkgd", weight, values, preferred_element_type=jnp.float32)
    attn = attn + own_weight[..., None] * own_value[:, :, None, :]
    return attn.astype(jnp.bfloat16).reshape(slot_dev, kv_local * group * HEAD_DIM)


def exchange(blocks, axes):
    return lax.all_to_all(blocks, axes, 0, 0, tiled=True)


def spread(block, axes):
    count = 1
    for axis in axes if isinstance(axes, tuple) else (axes,):
        count *= lax.axis_size(axis)
    return exchange(jnp.broadcast_to(block[None], (count, *block.shape)), axes)


def other_core(value):
    return lax.ppermute(value, "dp_2", [(0, 1), (1, 0)])


def inverse_rms(rows):
    return lax.rsqrt(jnp.mean(rows * rows, axis=-1, keepdims=True) + 1e-06)


def product(rows, slots):
    return lax.dot_general(
        rows, slots, (((1,), (1,)), ((), ())), preferred_element_type=jnp.float32
    )


def load_rows(own_hbm, other_hbm, column, width, weights, sems):
    copies = []
    for which, source in enumerate((own_hbm, other_hbm)):
        for tile in range(own_hbm.shape[0] // TILE):
            place = which * (own_hbm.shape[0] // TILE) + tile
            copy = pltpu.make_async_copy(
                source.at[pl.ds(tile * TILE, TILE), pl.ds(column, width)],
                weights.at[place],
                sems.at[place],
            )
            copy.start()
            copies.append(copy)
    return copies


def first_half_kernel(every_hbm, own_hbm, other_hbm, part_hbm, every, weights, part, in_sem, out_sem, sems):
    width = every.shape[1]
    load = pltpu.make_async_copy(every_hbm, every, in_sem)
    load.start()
    copies = load_rows(own_hbm, other_hbm, 0, width, weights, sems)
    load.wait()
    stores = []
    for place, copy in enumerate(copies):
        copy.wait()
        part[place] = product(weights[place], every[...])
        store = pltpu.make_async_copy(part.at[place], part_hbm.at[place], out_sem.at[place])
        store.start()
        stores.append(store)
    for store in stores:
        store.wait()


def first_half(every, own, other):
    slots, width = every.shape
    rows = own.shape[0]
    tiles = 2 * rows // TILE
    hbm = pl.BlockSpec(memory_space=pltpu.HBM)
    return pl.pallas_call(
        first_half_kernel,
        in_specs=[hbm, hbm, hbm],
        out_specs=hbm,
        out_shape=jax.ShapeDtypeStruct((tiles, TILE, slots), jnp.float32),
        scratch_shapes=[
            pltpu.VMEM((slots, width), jnp.bfloat16),
            pltpu.VMEM((tiles, TILE, width), jnp.bfloat16),
            pltpu.VMEM((tiles, TILE, slots), jnp.float32),
            pltpu.SemaphoreType.DMA,
            pltpu.SemaphoreType.DMA((tiles,)),
            pltpu.SemaphoreType.DMA((tiles,)),
        ],
        compiler_params=pltpu.CompilerParams(vmem_limit_bytes=VMEM_GRANT),
        cost_estimate=pl.CostEstimate(
            flops=4 * rows * slots * width, bytes_accessed=4 * rows * width, transcendentals=0
        ),
        name="first_half",
    )(every, own, other)


def second_half_kernel(
    starts_ref, every_hbm, own_hbm, other_hbm, part_hbm, out_ref, every, weights, part, in_sem, sems, part_sems
):
    tiles, _, width = weights.shape
    half_tiles = tiles // 2
    slots = every.shape[0]
    load = pltpu.make_async_copy(every_hbm, every, in_sem)
    load.start()
    copies = load_rows(own_hbm, other_hbm, width, width, weights, sems)
    parts = []
    for place in range(tiles):
        copy = pltpu.make_async_copy(part_hbm.at[place], part.at[place], part_sems.at[place])
        copy.start()
        parts.append(copy)
    load.wait()
    lane = lax.broadcasted_iota(jnp.int32, (16, META), 1)
    row = lax.broadcasted_iota(jnp.int32, (16, META), 0)
    digit = jnp.where(lane == 0, 1.0, jnp.where(lane == 1, 64.0, jnp.where(lane == 2, 4096.0, 0.0)))
    pick = jnp.where(row == 0, digit, jnp.where(lane == row + 2, 1.0, 0.0))
    notes = product(pick.astype(jnp.bfloat16), every[:, width:])
    ids = notes[0:1, :].astype(jnp.int32)
    line = lax.broadcasted_iota(jnp.int32, (TILE, slots), 0)
    top = jnp.full((1, slots), -jnp.inf, jnp.float32)
    total = jnp.zeros((1, slots), jnp.float32)
    picked = jnp.zeros((1, slots), jnp.float32)
    for place in range(tiles):
        copies[place].wait()
        parts[place].wait()
        logits = part[place] + product(weights[place], every[:, :width])
        part[place] = logits
        begin = starts_ref[place // half_tiles] + (place % half_tiles) * TILE
        picked = picked + jnp.sum(jnp.where(line == ids - begin, logits, 0.0), axis=0, keepdims=True)
        higher = jnp.maximum(top, jnp.max(logits, axis=0, keepdims=True))
        total = total * jnp.exp(top - higher) + jnp.sum(
            jnp.exp(logits - higher), axis=0, keepdims=True
        )
        top = higher
    out_ref[0:1, :] = top + jnp.log(total)
    out_ref[1:2, :] = picked
    out_ref[2:8, :] = notes[1:7, :]


def second_half(starts, every, own, other, part):
    slots, wide = every.shape
    width = wide - META
    rows = own.shape[0]
    tiles = 2 * rows // TILE
    hbm = pl.BlockSpec(memory_space=pltpu.HBM)
    return pl.pallas_call(
        second_half_kernel,
        in_specs=[pl.BlockSpec(memory_space=pltpu.SMEM), hbm, hbm, hbm, hbm],
        out_specs=pl.BlockSpec(memory_space=pltpu.VMEM),
        out_shape=jax.ShapeDtypeStruct((8, slots), jnp.float32),
        scratch_shapes=[
            pltpu.VMEM((slots, wide), jnp.bfloat16),
            pltpu.VMEM((tiles, TILE, width), jnp.bfloat16),
            pltpu.VMEM((tiles, TILE, slots), jnp.float32),
            pltpu.SemaphoreType.DMA,
            pltpu.SemaphoreType.DMA((tiles,)),
            pltpu.SemaphoreType.DMA((tiles,)),
        ],
        compiler_params=pltpu.CompilerParams(vmem_limit_bytes=LAST_GRANT),
        cost_estimate=pl.CostEstimate(
            flops=4 * rows * slots * width,
            bytes_accessed=4 * rows * width,
            transcendentals=2 * rows * slots,
        ),
        name="second_half",
    )(starts, every, own, other, part)


def on_device(
    query,
    incoming_key,
    new_value,
    key_cache,
    value_cache,
    cache_len,
    out_weight,
    residual,
    post_gain,
    final_gain,
    vocab_weight,
    sampled,
    stop_flag,
):
    slot_dev = query.shape[0]
    nz = lax.axis_size("tensor")
    z = lax.axis_index("tensor")
    core = lax.axis_index("dp_2")
    plane = lax.axis_index(PLANE)
    planes = lax.axis_size(PLANE)
    freed = (stop_flag == 1).astype(jnp.int32)
    count = jnp.sum(freed)

    vocab_other = other_core(vocab_weight)
    count_other = other_core(jnp.broadcast_to(count.astype(jnp.float32), (8, 128)))[0, 0]

    attn = attend_local(query, incoming_key, new_value, key_cache, value_cache, cache_len)
    partial_value = jnp.dot(attn, out_weight, preferred_element_type=jnp.float32)
    per = slot_dev // nz
    pieces = exchange(partial_value.astype(jnp.bfloat16).reshape(nz, per, D), "tensor")
    proj = jnp.sum(pieces.astype(jnp.float32), axis=0)
    post = proj * inverse_rms(proj) * post_gain
    own_residual = lax.dynamic_slice_in_dim(residual, z * per, per, 0)
    mix = (own_residual.astype(jnp.float32) + post).astype(jnp.bfloat16)
    full_mix = spread(mix, "tensor").reshape(slot_dev, D)
    mixed = full_mix.astype(jnp.float32)
    hidden = (mixed * inverse_rms(mixed) * final_gain).astype(jnp.bfloat16)
    width = D // nz
    new_residual = lax.dynamic_slice_in_dim(full_mix, z * width, width, 1)

    meta = jnp.stack(
        [
            sampled & 63,
            (sampled >> 6) & 63,
            sampled >> 12,
            freed,
            jnp.broadcast_to(count_other.astype(jnp.int32), (slot_dev,)),
        ],
        axis=1,
    ).astype(jnp.bfloat16)
    meta = jnp.pad(meta, ((0, 0), (0, META - meta.shape[1])))
    half = D // 2
    slots = planes * slot_dev
    every_a = spread(hidden[:, :half], PLANE).reshape(slots, half)
    every_b = spread(jnp.concatenate([hidden[:, half:], meta], axis=1), PLANE)
    every_b = every_b.reshape(slots, half + META)

    per_device = vocab_weight.shape[0]
    start = (lax.axis_index(DP) * nz + z) * per_device
    start_other = ((plane * 2 + 1 - core) * nz + z) * per_device
    part = first_half(every_a, vocab_weight, vocab_other)
    stats = second_half(
        jnp.stack([start, start_other]), every_b, vocab_weight, vocab_other, part
    )
    pair = stats[:2].reshape(2, planes, slot_dev).transpose(1, 0, 2).reshape(planes, 1, 2 * slot_dev)
    pair = jnp.broadcast_to(pair, (planes, nz, 2 * slot_dev)).reshape(planes * nz, 2 * slot_dev)
    gathered = exchange(pair, CHIPS)
    parts = gathered[:, :slot_dev]
    highest = jnp.max(parts, axis=0)
    overall = jnp.log(jnp.sum(jnp.exp(parts - highest[None]), axis=0)) + highest
    token_logprob = jnp.sum(gathered[:, slot_dev:], axis=0) - overall

    notes = stats[2:4].astype(jnp.int32).reshape(2, planes, slot_dev)
    counts_here = jnp.sum(notes[0], axis=1)
    counts_there = notes[1][:, 0]
    chips = jnp.arange(planes, dtype=jnp.int32)
    both = counts_here + counts_there
    before = jnp.sum(jnp.where(chips < plane, both, 0))
    before = before + jnp.where(core == 1, count_other.astype(jnp.int32), 0)
    released = jnp.sum(both).astype(jnp.int32)
    insert_rank = jnp.where(freed == 1, jnp.cumsum(freed) - freed + before, -1)
    return (new_residual, token_logprob, insert_rank.astype(jnp.int32), released)


def solution(mesh):
    split = Mesh(
        mesh.devices.reshape(4, 4, 2, mesh.shape["tensor"]), ("dp_0", "dp_1", "dp_2", "tensor")
    )
    in_specs = (
        P(DP, "tensor"),
        P(DP, "tensor"),
        P(DP, "tensor"),
        P(DP, None, "tensor"),
        P(DP, None, "tensor"),
        P(DP),
        P("tensor", None),
        P(DP, None),
        P(),
        P(),
        P(DP_TENSOR, None),
        P(DP),
        P(DP),
    )
    out_specs = (P(DP, "tensor"), P(DP), P(DP), P())
    return jax.shard_map(
        on_device, mesh=split, in_specs=in_specs, out_specs=out_specs, check_vma=False
    )
```

```python
import jax
import jax.numpy as jnp
from jax import lax
from jax.experimental import pallas as pl
from jax.experimental.pallas import tpu as pltpu
from jax.sharding import Mesh
from jax.sharding import PartitionSpec as P

D = 4608
HEADS = 32
KV_HEADS = 16
HEAD_DIM = 128
DP = ("dp_0", "dp_1", "dp_2")
DP_TENSOR = ("dp_0", "dp_1", "dp_2", "tensor")
PLANE = ("dp_0", "dp_1")
CHIPS = ("dp_0", "dp_1", "tensor")
META = 128


def attend_local(query, incoming_key, new_value, key_cache, value_cache, cache_len):
    slot_dev = query.shape[0]
    positions = key_cache.shape[1]
    kv_local = incoming_key.shape[1] // HEAD_DIM
    group = HEADS // KV_HEADS
    query_vector = query.reshape(slot_dev, kv_local, group, HEAD_DIM)
    keys = key_cache.reshape(slot_dev, positions, kv_local, HEAD_DIM)
    values = value_cache.reshape(slot_dev, positions, kv_local, HEAD_DIM)
    self_key = incoming_key.reshape(slot_dev, kv_local, HEAD_DIM)
    own_value = new_value.reshape(slot_dev, kv_local, HEAD_DIM).astype(jnp.float32)
    scores = (
        jnp.einsum("bkgd,bckd->bkgc", query_vector, keys, preferred_element_type=jnp.float32) / 12.0
    )
    self_entry = (
        jnp.einsum("qyxm,qym->qyx", query_vector, self_key, preferred_element_type=jnp.float32)
        / 12.0
    )
    valid = (
        jnp.arange(positions, dtype=jnp.int32)[None, None, None, :] < cache_len[:, None, None, None]
    )
    scores = jnp.where(valid, scores, -1e30)
    top = jnp.maximum(jnp.max(scores, axis=-1), self_entry)
    expo = jnp.where(valid, jnp.exp(scores - top[..., None]), 0.0)
    own_exp = jnp.exp(self_entry - top)
    total = jnp.sum(expo, axis=-1) + own_exp
    weight = (expo / total[..., None]).astype(jnp.bfloat16)
    own_weight = (own_exp / total).astype(jnp.bfloat16).astype(jnp.float32)
    attn = jnp.einsum("bkgc,bckd->bkgd", weight, values, preferred_element_type=jnp.float32)
    attn = attn + own_weight[..., None] * own_value[:, :, None, :]
    return attn.astype(jnp.bfloat16).reshape(slot_dev, kv_local * group * HEAD_DIM)


def exchange(blocks, axes):
    return lax.all_to_all(blocks, axes, 0, 0, tiled=True)


def other_core(value):
    return lax.ppermute(value, "dp_2", [(0, 1), (1, 0)])


def inverse_rms(rows):
    return lax.rsqrt(jnp.mean(rows * rows, axis=-1, keepdims=True) + 1e-06)


def product(rows, slots):
    return lax.dot_general(
        rows, slots, (((1,), (1,)), ((), ())), preferred_element_type=jnp.float32
    )


def in_vmem(count):
    return [pl.BlockSpec(memory_space=pltpu.VMEM)] * count


def params(mib):
    return pltpu.CompilerParams(vmem_limit_bytes=mib * 1024 * 1024)


def mix_kernel(pieces_ref, residual_ref, gain_ref, out_ref):
    nz, per, _ = pieces_ref.shape
    z = lax.axis_index("tensor")
    proj = pieces_ref[0].astype(jnp.float32)
    for k in range(1, nz):
        proj = proj + pieces_ref[k].astype(jnp.float32)
    post = proj * inverse_rms(proj) * gain_ref[...]
    residual = residual_ref[...].astype(jnp.float32)
    row = lax.broadcasted_iota(jnp.int32, (residual.shape[0], 1), 0)
    picked = [
        jnp.sum(jnp.where(row == z * per + k, residual, 0.0), axis=0, keepdims=True)
        for k in range(per)
    ]
    mix = (jnp.concatenate(picked, axis=0) + post).astype(jnp.bfloat16)
    for k in range(nz):
        out_ref[k] = mix


def mix_rows(pieces, residual, gain):
    return pl.pallas_call(
        mix_kernel,
        in_specs=in_vmem(3),
        out_specs=in_vmem(1)[0],
        out_shape=jax.ShapeDtypeStruct(pieces.shape, jnp.bfloat16),
        compiler_params=params(4),
        name="mix_rows",
    )(pieces, residual, gain)


def as_column(line):
    size = line.shape[1]
    row = lax.broadcasted_iota(jnp.int32, (size, size), 0)
    lane = lax.broadcasted_iota(jnp.int32, (size, size), 1)
    return jnp.sum(jnp.where(row == lane, line, 0), axis=1, keepdims=True)


def hidden_kernel(mix_ref, gain_ref, sampled_ref, flag_ref, other_ref, block_ref, slice_ref, rows):
    nz, per, _ = mix_ref.shape
    slot_dev, width = slice_ref.shape
    z = lax.axis_index("tensor")
    for k in range(nz):
        rows[k * per : (k + 1) * per, :] = mix_ref[k].astype(jnp.float32)
    mixed = rows[...]
    hidden = (mixed * inverse_rms(mixed) * gain_ref[...]).astype(jnp.bfloat16)
    sampled = sampled_ref[...]
    freed = (flag_ref[...] == 1).astype(jnp.int32)
    count = jnp.sum((other_ref[...] == 1).astype(jnp.int32), axis=1, keepdims=True)
    values = [sampled & 63, (sampled >> 6) & 63, sampled >> 12, freed]
    lane = lax.broadcasted_iota(jnp.int32, (slot_dev, META), 1)
    notes = jnp.where(lane == 4, count, 0)
    for k, value in enumerate(values):
        notes = jnp.where(lane == k, as_column(value), notes)
    notes = notes.astype(jnp.float32).astype(jnp.bfloat16)
    for k in range(block_ref.shape[0]):
        block_ref[k, :, :D] = hidden
        block_ref[k, :, D:] = notes
    for k in range(nz):

        @pl.when(z == k)
        def _():
            slice_ref[...] = rows[:, k * width : (k + 1) * width].astype(jnp.bfloat16)


def hidden_blocks(mix, gain, sampled, flag, other_flag, planes):
    slot_dev = mix.shape[0] * mix.shape[1]
    width = D // mix.shape[0]
    return pl.pallas_call(
        hidden_kernel,
        in_specs=in_vmem(5),
        out_specs=in_vmem(2),
        out_shape=[
            jax.ShapeDtypeStruct((planes, slot_dev, D + META), jnp.bfloat16),
            jax.ShapeDtypeStruct((slot_dev, width), jnp.bfloat16),
        ],
        scratch_shapes=[pltpu.VMEM((slot_dev, D), jnp.float32)],
        compiler_params=params(8),
        name="hidden_blocks",
    )(mix, gain, sampled, flag, other_flag)


def vocab_kernel(every_ref, own_ref, other_ref, flag_ref, pair_ref, rank_ref, total_ref):
    slots = every_ref.shape[0]
    per_device = own_ref.shape[0]
    slot_dev = flag_ref.shape[1]
    planes = slots // slot_dev
    nz = pair_ref.shape[0] // planes
    z = lax.axis_index("tensor")
    core = lax.axis_index("dp_2")
    plane = lax.axis_index("dp_0") * lax.axis_size("dp_1") + lax.axis_index("dp_1")
    every = every_ref[:, :D]
    lane = lax.broadcasted_iota(jnp.int32, (16, META), 1)
    row = lax.broadcasted_iota(jnp.int32, (16, META), 0)
    digit = jnp.where(lane == 0, 1.0, jnp.where(lane == 1, 64.0, jnp.where(lane == 2, 4096.0, 0.0)))
    pick = jnp.where(row == 0, digit, jnp.where(lane == row + 2, 1.0, 0.0))
    notes = product(pick.astype(jnp.bfloat16), every_ref[:, D:])
    ids = notes[0:1, :].astype(jnp.int32)
    line = lax.broadcasted_iota(jnp.int32, (per_device, slots), 0)
    tops, sums = [], []
    picked = jnp.zeros((1, slots), jnp.float32)
    for weight_ref, holder in ((own_ref, core), (other_ref, 1 - core)):
        begin = ((plane * 2 + holder) * nz + z) * per_device
        logits = product(weight_ref[...], every)
        picked = picked + jnp.sum(jnp.where(line == ids - begin, logits, 0.0), axis=0, keepdims=True)
        top = jnp.max(logits, axis=0, keepdims=True)
        tops.append(top)
        sums.append(jnp.sum(jnp.exp(logits - top), axis=0, keepdims=True))
    top = jnp.maximum(tops[0], tops[1])
    total = sums[0] * jnp.exp(tops[0] - top) + sums[1] * jnp.exp(tops[1] - top)
    entropy = top + jnp.log(total)
    for k in range(planes):
        for part, value in ((0, entropy), (1, picked)):
            pair_ref[k * nz : (k + 1) * nz, part * slot_dev : (part + 1) * slot_dev] = (
                jnp.broadcast_to(value[:, k * slot_dev : (k + 1) * slot_dev], (nz, slot_dev))
            )

    slot = lax.broadcasted_iota(jnp.int32, (1, slots), 1)
    flags = notes[1:2, :]
    counts = jnp.where(slot % slot_dev == 0, notes[2:3, :], 0.0)
    both = flags + counts
    total_ref[...] = jnp.sum(both, axis=1, keepdims=True).astype(jnp.int32)
    before = jnp.sum(jnp.where(slot // slot_dev < plane, both, 0.0), axis=1, keepdims=True)
    partner = jnp.sum(jnp.where(slot == plane * slot_dev, counts, 0.0), axis=1, keepdims=True)
    before = (before + jnp.where(core == 1, partner, 0.0)).astype(jnp.int32)
    freed = (flag_ref[...] == 1).astype(jnp.int32)
    below = lax.broadcasted_iota(jnp.int32, (slot_dev, slot_dev), 0)
    place = lax.broadcasted_iota(jnp.int32, (slot_dev, slot_dev), 1)
    ahead = jnp.sum(jnp.where(below < place, as_column(freed), 0), axis=0, keepdims=True)
    rank_ref[...] = jnp.where(freed == 1, ahead + before, -1)


def vocab_stats(every, own, other, flag, nz):
    slots = every.shape[0]
    rows = own.shape[0]
    slot_dev = flag.shape[1]
    return pl.pallas_call(
        vocab_kernel,
        in_specs=in_vmem(4),
        out_specs=in_vmem(3),
        out_shape=[
            jax.ShapeDtypeStruct((slots // slot_dev * nz, 2 * slot_dev), jnp.float32),
            jax.ShapeDtypeStruct((1, slot_dev), jnp.int32),
            jax.ShapeDtypeStruct((1, 1), jnp.int32),
        ],
        compiler_params=params(24),
        cost_estimate=pl.CostEstimate(
            flops=4 * rows * slots * D, bytes_accessed=4 * rows * D, transcendentals=2 * rows * slots
        ),
        name="vocab_stats",
    )(every, own, other, flag)


def on_device(
    query,
    incoming_key,
    new_value,
    key_cache,
    value_cache,
    cache_len,
    out_weight,
    residual,
    post_gain,
    final_gain,
    vocab_weight,
    sampled,
    stop_flag,
):
    slot_dev = query.shape[0]
    nz = lax.axis_size("tensor")
    planes = lax.axis_size(PLANE)
    vocab_other = other_core(vocab_weight)
    other_flag = other_core(stop_flag)

    attn = attend_local(query, incoming_key, new_value, key_cache, value_cache, cache_len)
    partial_value = jnp.dot(attn, out_weight, preferred_element_type=jnp.float32)
    blocks = partial_value.astype(jnp.bfloat16).reshape(nz, slot_dev // nz, D)
    post_line, final_line = post_gain.reshape(1, D), final_gain.reshape(1, D)
    flag, sampled_line = stop_flag.reshape(1, slot_dev), sampled.reshape(1, slot_dev)
    blocks, vocab_other, other_flag, post_line, final_line, flag, sampled_line = (
        lax.optimization_barrier(
            (blocks, vocab_other, other_flag, post_line, final_line, flag, sampled_line)
        )
    )
    pieces = exchange(blocks, "tensor")
    mix = exchange(mix_rows(pieces, residual, post_line), "tensor")
    hidden, new_residual = hidden_blocks(
        mix,
        final_line,
        sampled_line,
        flag,
        other_flag.reshape(1, slot_dev),
        planes,
    )
    every = exchange(hidden, PLANE).reshape(planes * slot_dev, D + META)
    pair, rank, released = vocab_stats(every, vocab_weight, vocab_other, flag, nz)
    gathered = exchange(pair, CHIPS)
    parts = gathered[:, :slot_dev]
    highest = jnp.max(parts, axis=0)
    overall = jnp.log(jnp.sum(jnp.exp(parts - highest[None]), axis=0)) + highest
    token_logprob = jnp.sum(gathered[:, slot_dev:], axis=0) - overall
    return (new_residual, token_logprob, rank.reshape(slot_dev), released.reshape(()))


def solution(mesh):
    split = Mesh(
        mesh.devices.reshape(4, 4, 2, mesh.shape["tensor"]), ("dp_0", "dp_1", "dp_2", "tensor")
    )
    in_specs = (
        P(DP, "tensor"),
        P(DP, "tensor"),
        P(DP, "tensor"),
        P(DP, None, "tensor"),
        P(DP, None, "tensor"),
        P(DP),
        P("tensor", None),
        P(DP, None),
        P(),
        P(),
        P(DP_TENSOR, None),
        P(DP),
        P(DP),
    )
    out_specs = (P(DP, "tensor"), P(DP), P(DP), P())
    return jax.shard_map(
        on_device, mesh=split, in_specs=in_specs, out_specs=out_specs, check_vma=False
    )
```

```python
import jax
import jax.numpy as jnp
from jax import lax
from jax.experimental import pallas as pl
from jax.experimental.pallas import tpu as pltpu
from jax.sharding import Mesh
from jax.sharding import PartitionSpec as P

D = 4608
HEADS = 32
KV_HEADS = 16
HEAD_DIM = 128
DP = ("dp_0", "dp_1", "dp_2")
DP_TENSOR = ("dp_0", "dp_1", "dp_2", "tensor")
PLANE = ("dp_0", "dp_1")
CHIPS = ("dp_0", "dp_1", "tensor")
META = 128
CHUNKS = 4


def attend_kernel(
    len_ref, query_hbm, key_hbm, value_hbm, keys_hbm, values_hbm, weight_hbm, out_hbm,
    keys, values, weight, query_ref, key_ref, value_ref, out_ref,
    query_s, key_s, value_s, score_s, attn_s, part_s, key_sem, value_sem, weight_sem, small_sem,
):
    slot_dev = keys.shape[0]
    positions = keys.shape[1]
    group = HEADS // KV_HEADS
    heads = query_ref.shape[1] // HEAD_DIM
    kv_local = heads // group
    batch = slot_dev // key_sem.shape[0]
    chunk = D // weight_sem.shape[0]
    loads = {}
    smalls = ((query_hbm, query_ref), (key_hbm, key_ref), (value_hbm, value_ref))
    for k, (source, target) in enumerate(smalls):
        loads["s", k] = pltpu.make_async_copy(source, target, small_sem.at[k])
        loads["s", k].start()
    for name, source, target, sem in (("k", keys_hbm, keys, key_sem), ("v", values_hbm, values, value_sem)):
        for k in range(sem.shape[0]):
            part = pl.ds(k * batch, batch)
            loads[name, k] = pltpu.make_async_copy(source.at[part], target.at[part], sem.at[k])
            loads[name, k].start()
    for k in range(weight_sem.shape[0]):
        part = pl.ds(k * chunk, chunk)
        loads["w", k] = pltpu.make_async_copy(
            weight_hbm.at[:, part], weight.at[:, part], weight_sem.at[k]
        )
        loads["w", k].start()

    for k in range(len(smalls)):
        loads["s", k].wait()
    for h in range(heads):
        at = pl.ds(h, slot_dev, stride=heads)
        kv = h // group * HEAD_DIM
        query_s[at, :] = query_ref[:, h * HEAD_DIM : (h + 1) * HEAD_DIM].astype(jnp.float32)
        key_s[at, :] = key_ref[:, kv : kv + HEAD_DIM].astype(jnp.float32)
        value_s[at, :] = value_ref[:, kv : kv + HEAD_DIM].astype(jnp.float32)

    lines = 8
    pair = lines // heads
    row = lax.broadcasted_iota(jnp.int32, (lines, 1), 0)
    kind = row % heads // group

    def per_slot(rows, source, first, contract):
        found = None
        for k in range(pair):
            part = lax.dot_general(
                rows, source[first + k], (((1,), (contract,)), ((), ())), preferred_element_type=jnp.float32
            )
            found = part if found is None else jnp.where(row >= k * heads, part, found)
        return found

    for i in range(slot_dev // pair):
        if i * pair % batch == 0:
            loads["k", i * pair // batch].wait()
        rows = query_s[i * lines : (i + 1) * lines, :]
        spread = [jnp.where(kind == k, rows, 0.0) for k in range(kv_local)]
        spread = jnp.concatenate(spread, axis=1).astype(jnp.bfloat16)
        score_s[i * lines : (i + 1) * lines, :] = per_slot(spread, keys, i * pair, 1)

    total_rows = slot_dev * heads
    owner = lax.broadcasted_iota(jnp.int32, (total_rows, 1), 0) // heads
    length = jnp.zeros((total_rows, 1), jnp.int32)
    for k in range(slot_dev):
        length = jnp.where(owner == k, len_ref[k], length)
    valid = lax.broadcasted_iota(jnp.int32, (total_rows, positions), 1) < length
    scores = jnp.where(valid, score_s[...] / 12.0, -1e30)
    own = jnp.sum(query_s[...] * key_s[...], axis=1, keepdims=True) / 12.0
    top = jnp.maximum(jnp.max(scores, axis=1, keepdims=True), own)
    expo = jnp.where(valid, jnp.exp(scores - top), 0.0)
    own_exp = jnp.exp(own - top)
    total = jnp.sum(expo, axis=1, keepdims=True) + own_exp
    score_s[...] = expo / total
    own_weight = (own_exp / total).astype(jnp.bfloat16).astype(jnp.float32)

    for i in range(slot_dev // pair):
        if i * pair % batch == 0:
            loads["v", i * pair // batch].wait()
        rows = score_s[i * lines : (i + 1) * lines, :].astype(jnp.bfloat16)
        mixed = per_slot(rows, values, i * pair, 0)
        found = mixed[:, :HEAD_DIM]
        for k in range(1, kv_local):
            found = jnp.where(kind == k, mixed[:, k * HEAD_DIM : (k + 1) * HEAD_DIM], found)
        attn_s[i * lines : (i + 1) * lines, :] = found
    attn_s[...] += own_weight * value_s[...]
    attn = [attn_s[pl.ds(h, slot_dev, stride=heads), :] for h in range(heads)]
    attn = jnp.concatenate(attn, axis=1).astype(jnp.bfloat16)
    for k in range(weight_sem.shape[0]):
        loads["w", k].wait()
        part_s[:, k * chunk : (k + 1) * chunk] = jnp.dot(
            attn, weight[:, k * chunk : (k + 1) * chunk], preferred_element_type=jnp.float32
        )
    per = out_ref.shape[1]
    for k in range(out_ref.shape[0]):
        out_ref[k] = part_s[k * per : (k + 1) * per, :].astype(jnp.bfloat16)
    store = pltpu.make_async_copy(out_ref, out_hbm, small_sem.at[0])
    store.start()
    store.wait()


def attend(query, incoming_key, new_value, key_cache, value_cache, cache_len, out_weight, nz):
    slot_dev = query.shape[0]
    lines = slot_dev * (query.shape[1] // HEAD_DIM)
    hbm = pl.BlockSpec(memory_space=pltpu.HBM)
    return pl.pallas_call(
        attend_kernel,
        in_specs=[pl.BlockSpec(memory_space=pltpu.SMEM), *[hbm] * 6],
        out_specs=hbm,
        out_shape=jax.ShapeDtypeStruct((nz, slot_dev // nz, D), jnp.bfloat16),
        scratch_shapes=[
            pltpu.VMEM(key_cache.shape, jnp.bfloat16),
            pltpu.VMEM(value_cache.shape, jnp.bfloat16),
            pltpu.VMEM(out_weight.shape, jnp.bfloat16),
            pltpu.VMEM(query.shape, jnp.bfloat16),
            pltpu.VMEM(incoming_key.shape, jnp.bfloat16),
            pltpu.VMEM(new_value.shape, jnp.bfloat16),
            pltpu.VMEM((nz, slot_dev // nz, D), jnp.bfloat16),
            *[pltpu.VMEM((lines, HEAD_DIM), jnp.float32)] * 3,
            pltpu.VMEM((lines, key_cache.shape[1]), jnp.float32),
            pltpu.VMEM((lines, HEAD_DIM), jnp.float32),
            pltpu.VMEM((slot_dev, D), jnp.float32),
            pltpu.SemaphoreType.DMA((4,)),
            pltpu.SemaphoreType.DMA((4,)),
            pltpu.SemaphoreType.DMA((4,)),
            pltpu.SemaphoreType.DMA((3,)),
        ],
        compiler_params=params(61),
        cost_estimate=pl.CostEstimate(flops=2_000_000_000, bytes_accessed=9_000_000, transcendentals=20_000),
        name="attend",
    )(cache_len, query, incoming_key, new_value, key_cache, value_cache, out_weight)


def exchange(blocks, axes):
    return lax.all_to_all(blocks, axes, 0, 0, tiled=True)


def other_core(value):
    return lax.ppermute(value, "dp_2", [(0, 1), (1, 0)])


def inverse_rms(rows):
    return lax.rsqrt(jnp.mean(rows * rows, axis=-1, keepdims=True) + 1e-06)


def product(rows, slots):
    return lax.dot_general(
        rows, slots, (((1,), (1,)), ((), ())), preferred_element_type=jnp.float32
    )


def in_vmem(count):
    return [pl.BlockSpec(memory_space=pltpu.VMEM)] * count


def params(mib):
    return pltpu.CompilerParams(vmem_limit_bytes=mib * 1024 * 1024)


def mix_kernel(pieces_ref, residual_ref, gain_ref, out_ref):
    nz, per, _ = pieces_ref.shape
    z = lax.axis_index("tensor")
    proj = pieces_ref[0].astype(jnp.float32)
    for k in range(1, nz):
        proj = proj + pieces_ref[k].astype(jnp.float32)
    post = proj * inverse_rms(proj) * gain_ref[...].reshape(1, D)
    residual = residual_ref[...].astype(jnp.float32)
    row = lax.broadcasted_iota(jnp.int32, (residual.shape[0], 1), 0)
    picked = [
        jnp.sum(jnp.where(row == z * per + k, residual, 0.0), axis=0, keepdims=True)
        for k in range(per)
    ]
    mix = (jnp.concatenate(picked, axis=0) + post).astype(jnp.bfloat16)
    for k in range(nz):
        out_ref[k] = mix


def mix_rows(pieces, residual, gain):
    return pl.pallas_call(
        mix_kernel,
        in_specs=in_vmem(3),
        out_specs=in_vmem(1)[0],
        out_shape=jax.ShapeDtypeStruct(pieces.shape, jnp.bfloat16),
        compiler_params=params(4),
        name="mix_rows",
    )(pieces, residual, gain)


def as_column(line):
    size = line.shape[1]
    row = lax.broadcasted_iota(jnp.int32, (size, size), 0)
    lane = lax.broadcasted_iota(jnp.int32, (size, size), 1)
    return jnp.sum(jnp.where(row == lane, line, 0), axis=1, keepdims=True)


def hidden_kernel(mix_ref, gain_ref, sampled_ref, flag_ref, other_ref, block_ref, slice_ref, rows):
    nz, per, _ = mix_ref.shape
    slot_dev, width = slice_ref.shape
    z = lax.axis_index("tensor")
    for k in range(nz):
        rows[k * per : (k + 1) * per, :] = mix_ref[k].astype(jnp.float32)
    mixed = rows[...]
    hidden = (mixed * inverse_rms(mixed) * gain_ref[...].reshape(1, D)).astype(jnp.bfloat16)
    sampled = sampled_ref[...]
    freed = (flag_ref[...] == 1).astype(jnp.int32)
    count = jnp.sum((other_ref[...] == 1).astype(jnp.int32), axis=1, keepdims=True)
    values = [sampled & 63, (sampled >> 6) & 63, sampled >> 12, freed]
    lane = lax.broadcasted_iota(jnp.int32, (slot_dev, META), 1)
    notes = jnp.where(lane == 4, count, 0)
    for k, value in enumerate(values):
        notes = jnp.where(lane == k, as_column(value), notes)
    notes = notes.astype(jnp.float32).astype(jnp.bfloat16)
    for k in range(block_ref.shape[0]):
        block_ref[k, :, :D] = hidden
        block_ref[k, :, D:] = notes
    for k in range(nz):

        @pl.when(z == k)
        def _():
            slice_ref[...] = rows[:, k * width : (k + 1) * width].astype(jnp.bfloat16)


def hidden_blocks(mix, gain, sampled, flag, other_flag, planes):
    slot_dev = mix.shape[0] * mix.shape[1]
    width = D // mix.shape[0]
    return pl.pallas_call(
        hidden_kernel,
        in_specs=in_vmem(5),
        out_specs=in_vmem(2),
        out_shape=[
            jax.ShapeDtypeStruct((planes, slot_dev, D + META), jnp.bfloat16),
            jax.ShapeDtypeStruct((slot_dev, width), jnp.bfloat16),
        ],
        scratch_shapes=[pltpu.VMEM((slot_dev, D), jnp.float32)],
        compiler_params=params(8),
        name="hidden_blocks",
    )(mix, gain, sampled, flag, other_flag)


def vocab_kernel(
    every_ref, own_hbm, other_hbm, flag_ref, pair_ref, rank_ref, total_ref, weights, logits_s, sems
):
    slots = every_ref.shape[0]
    per_device = own_hbm.shape[0]
    chunk = weights.shape[2]
    loads = []
    for k in range(weights.shape[0]):
        for which, source in enumerate((own_hbm, other_hbm)):
            copy = pltpu.make_async_copy(
                source.at[:, pl.ds(k * chunk, chunk)],
                weights.at[k, pl.ds(which * per_device, per_device)],
                sems.at[k, which],
            )
            copy.start()
            loads.append(copy)
    slot_dev = flag_ref.shape[1]
    planes = slots // slot_dev
    nz = pair_ref.shape[0] // planes
    z = lax.axis_index("tensor")
    core = lax.axis_index("dp_2")
    plane = lax.axis_index("dp_0") * lax.axis_size("dp_1") + lax.axis_index("dp_1")
    lane = lax.broadcasted_iota(jnp.int32, (16, META), 1)
    row = lax.broadcasted_iota(jnp.int32, (16, META), 0)
    digit = jnp.where(lane == 0, 1.0, jnp.where(lane == 1, 64.0, jnp.where(lane == 2, 4096.0, 0.0)))
    pick = jnp.where(row == 0, digit, jnp.where(lane == row + 2, 1.0, 0.0))
    notes = product(pick.astype(jnp.bfloat16), every_ref[:, D:])
    ids = notes[0:1, :].astype(jnp.int32)
    for k in range(weights.shape[0]):
        loads[2 * k].wait()
        loads[2 * k + 1].wait()
        part = product(weights[k], every_ref[:, k * chunk : (k + 1) * chunk])
        logits_s[...] = part if k == 0 else logits_s[...] + part
    line = lax.broadcasted_iota(jnp.int32, (per_device, slots), 0)
    tops, sums = [], []
    picked = jnp.zeros((1, slots), jnp.float32)
    for which, holder in enumerate((core, 1 - core)):
        begin = ((plane * 2 + holder) * nz + z) * per_device
        logits = logits_s[which * per_device : (which + 1) * per_device, :]
        picked = picked + jnp.sum(jnp.where(line == ids - begin, logits, 0.0), axis=0, keepdims=True)
        top = jnp.max(logits, axis=0, keepdims=True)
        tops.append(top)
        sums.append(jnp.sum(jnp.exp(logits - top), axis=0, keepdims=True))
    top = jnp.maximum(tops[0], tops[1])
    total = sums[0] * jnp.exp(tops[0] - top) + sums[1] * jnp.exp(tops[1] - top)
    entropy = top + jnp.log(total)
    for k in range(planes):
        for part, value in ((0, entropy), (1, picked)):
            pair_ref[k * nz : (k + 1) * nz, part * slot_dev : (part + 1) * slot_dev] = (
                jnp.broadcast_to(value[:, k * slot_dev : (k + 1) * slot_dev], (nz, slot_dev))
            )

    slot = lax.broadcasted_iota(jnp.int32, (1, slots), 1)
    flags = notes[1:2, :]
    counts = jnp.where(slot % slot_dev == 0, notes[2:3, :], 0.0)
    both = flags + counts
    total_ref[...] = jnp.sum(both, axis=1, keepdims=True).astype(jnp.int32)
    before = jnp.sum(jnp.where(slot // slot_dev < plane, both, 0.0), axis=1, keepdims=True)
    partner = jnp.sum(jnp.where(slot == plane * slot_dev, counts, 0.0), axis=1, keepdims=True)
    before = (before + jnp.where(core == 1, partner, 0.0)).astype(jnp.int32)
    freed = (flag_ref[...] == 1).astype(jnp.int32)
    below = lax.broadcasted_iota(jnp.int32, (slot_dev, slot_dev), 0)
    place = lax.broadcasted_iota(jnp.int32, (slot_dev, slot_dev), 1)
    ahead = jnp.sum(jnp.where(below < place, as_column(freed), 0), axis=0, keepdims=True)
    rank_ref[...] = jnp.where(freed == 1, ahead + before, -1)


def vocab_stats(every, own, other, flag, nz):
    slots = every.shape[0]
    rows = own.shape[0]
    slot_dev = flag.shape[1]
    hbm = pl.BlockSpec(memory_space=pltpu.HBM)
    return pl.pallas_call(
        vocab_kernel,
        in_specs=[*in_vmem(1), hbm, hbm, *in_vmem(1)],
        out_specs=in_vmem(3),
        out_shape=[
            jax.ShapeDtypeStruct((slots // slot_dev * nz, 2 * slot_dev), jnp.float32),
            jax.ShapeDtypeStruct((1, slot_dev), jnp.int32),
            jax.ShapeDtypeStruct((1, 1), jnp.int32),
        ],
        scratch_shapes=[
            pltpu.VMEM((CHUNKS, 2 * rows, D // CHUNKS), jnp.bfloat16),
            pltpu.VMEM((2 * rows, slots), jnp.float32),
            pltpu.SemaphoreType.DMA((CHUNKS, 2)),
        ],
        compiler_params=params(50),
        cost_estimate=pl.CostEstimate(
            flops=4 * rows * slots * D, bytes_accessed=4 * rows * D, transcendentals=2 * rows * slots
        ),
        name="vocab_stats",
    )(every, own, other, flag)


def on_device(
    query,
    incoming_key,
    new_value,
    key_cache,
    value_cache,
    cache_len,
    out_weight,
    residual,
    post_gain,
    final_gain,
    vocab_weight,
    sampled,
    stop_flag,
):
    slot_dev = query.shape[0]
    nz = lax.axis_size("tensor")
    planes = lax.axis_size(PLANE)
    vocab_other = other_core(vocab_weight)
    other_flag = other_core(stop_flag)

    blocks = attend(
        query, incoming_key, new_value, key_cache, value_cache, cache_len, out_weight, nz
    )
    flag, sampled_line = stop_flag.reshape(1, slot_dev), sampled.reshape(1, slot_dev)
    blocks, vocab_other, other_flag, flag, sampled_line = lax.optimization_barrier(
        (blocks, vocab_other, other_flag, flag, sampled_line)
    )
    pieces = exchange(blocks, "tensor")
    mix = exchange(mix_rows(pieces, residual, post_gain), "tensor")
    hidden, new_residual = hidden_blocks(
        mix,
        final_gain,
        sampled_line,
        flag,
        other_flag.reshape(1, slot_dev),
        planes,
    )
    every = exchange(hidden, PLANE).reshape(planes * slot_dev, D + META)
    pair, rank, released = vocab_stats(every, vocab_weight, vocab_other, flag, nz)
    gathered = exchange(pair, CHIPS)
    parts = gathered[:, :slot_dev]
    highest = jnp.max(parts, axis=0)
    overall = jnp.log(jnp.sum(jnp.exp(parts - highest[None]), axis=0)) + highest
    token_logprob = jnp.sum(gathered[:, slot_dev:], axis=0) - overall
    return (new_residual, token_logprob, rank.reshape(slot_dev), released.reshape(()))


def solution(mesh):
    split = Mesh(
        mesh.devices.reshape(4, 4, 2, mesh.shape["tensor"]), ("dp_0", "dp_1", "dp_2", "tensor")
    )
    in_specs = (
        P(DP, "tensor"),
        P(DP, "tensor"),
        P(DP, "tensor"),
        P(DP, None, "tensor"),
        P(DP, None, "tensor"),
        P(DP),
        P("tensor", None),
        P(DP, None),
        P(),
        P(),
        P(DP_TENSOR, None),
        P(DP),
        P(DP),
    )
    out_specs = (P(DP, "tensor"), P(DP), P(DP), P())
    return jax.shard_map(
        on_device, mesh=split, in_specs=in_specs, out_specs=out_specs, check_vma=False
    )
```

```python
import jax
import jax.numpy as jnp
from jax import lax
from jax.experimental import pallas as pl
from jax.experimental.pallas import tpu as pltpu
from jax.sharding import Mesh
from jax.sharding import PartitionSpec as P

D = 4608
HEADS = 32
KV_HEADS = 16
HEAD_DIM = 128
DP = ("dp_0", "dp_1", "dp_2")
DP_TENSOR = ("dp_0", "dp_1", "dp_2", "tensor")
PLANE = ("dp_0", "dp_1")
CHIPS = ("dp_0", "dp_1", "tensor")
META = 128


def attend_kernel(
    len_ref, query_hbm, key_hbm, value_hbm, keys_hbm, values_hbm, weight_hbm, out_hbm,
    keys, values, weight, query_ref, key_ref, value_ref, out_ref,
    query_s, key_s, value_s, score_s, attn_s, part_s, key_sem, value_sem, weight_sem, small_sem,
):
    slot_dev = keys.shape[0]
    positions = keys.shape[1]
    group = HEADS // KV_HEADS
    heads = query_ref.shape[1] // HEAD_DIM
    kv_local = heads // group
    batch = slot_dev // key_sem.shape[0]
    chunk = D // weight_sem.shape[0]
    loads = {}
    smalls = ((query_hbm, query_ref), (key_hbm, key_ref), (value_hbm, value_ref))
    for k, (source, target) in enumerate(smalls):
        loads["s", k] = pltpu.make_async_copy(source, target, small_sem.at[k])
        loads["s", k].start()
    for name, source, target, sem in (("k", keys_hbm, keys, key_sem), ("v", values_hbm, values, value_sem)):
        for k in range(sem.shape[0]):
            part = pl.ds(k * batch, batch)
            loads[name, k] = pltpu.make_async_copy(source.at[part], target.at[part], sem.at[k])
            loads[name, k].start()
    for k in range(weight_sem.shape[0]):
        part = pl.ds(k * chunk, chunk)
        loads["w", k] = pltpu.make_async_copy(
            weight_hbm.at[:, part], weight.at[:, part], weight_sem.at[k]
        )
        loads["w", k].start()

    for k in range(len(smalls)):
        loads["s", k].wait()
    for h in range(heads):
        at = pl.ds(h, slot_dev, stride=heads)
        kv = h // group * HEAD_DIM
        query_s[at, :] = query_ref[:, h * HEAD_DIM : (h + 1) * HEAD_DIM].astype(jnp.float32)
        key_s[at, :] = key_ref[:, kv : kv + HEAD_DIM].astype(jnp.float32)
        value_s[at, :] = value_ref[:, kv : kv + HEAD_DIM].astype(jnp.float32)

    lines = 8
    pair = lines // heads
    row = lax.broadcasted_iota(jnp.int32, (lines, 1), 0)
    kind = row % heads // group

    def per_slot(rows, source, first, contract):
        found = None
        for k in range(pair):
            part = lax.dot_general(
                rows, source[first + k], (((1,), (contract,)), ((), ())), preferred_element_type=jnp.float32
            )
            found = part if found is None else jnp.where(row >= k * heads, part, found)
        return found

    for i in range(slot_dev // pair):
        if i * pair % batch == 0:
            loads["k", i * pair // batch].wait()
        rows = query_s[i * lines : (i + 1) * lines, :]
        spread = [jnp.where(kind == k, rows, 0.0) for k in range(kv_local)]
        spread = jnp.concatenate(spread, axis=1).astype(jnp.bfloat16)
        score_s[i * lines : (i + 1) * lines, :] = per_slot(spread, keys, i * pair, 1)

    total_rows = slot_dev * heads
    owner = lax.broadcasted_iota(jnp.int32, (total_rows, 1), 0) // heads
    length = jnp.zeros((total_rows, 1), jnp.int32)
    for k in range(slot_dev):
        length = jnp.where(owner == k, len_ref[k], length)
    valid = lax.broadcasted_iota(jnp.int32, (total_rows, positions), 1) < length
    scores = jnp.where(valid, score_s[...] / 12.0, -1e30)
    own = jnp.sum(query_s[...] * key_s[...], axis=1, keepdims=True) / 12.0
    top = jnp.maximum(jnp.max(scores, axis=1, keepdims=True), own)
    expo = jnp.where(valid, jnp.exp(scores - top), 0.0)
    own_exp = jnp.exp(own - top)
    total = jnp.sum(expo, axis=1, keepdims=True) + own_exp
    score_s[...] = expo / total
    own_weight = (own_exp / total).astype(jnp.bfloat16).astype(jnp.float32)

    for i in range(slot_dev // pair):
        if i * pair % batch == 0:
            loads["v", i * pair // batch].wait()
        rows = score_s[i * lines : (i + 1) * lines, :].astype(jnp.bfloat16)
        mixed = per_slot(rows, values, i * pair, 0)
        found = mixed[:, :HEAD_DIM]
        for k in range(1, kv_local):
            found = jnp.where(kind == k, mixed[:, k * HEAD_DIM : (k + 1) * HEAD_DIM], found)
        attn_s[i * lines : (i + 1) * lines, :] = found
    attn_s[...] += own_weight * value_s[...]
    attn = [attn_s[pl.ds(h, slot_dev, stride=heads), :] for h in range(heads)]
    attn = jnp.concatenate(attn, axis=1).astype(jnp.bfloat16)
    for k in range(weight_sem.shape[0]):
        loads["w", k].wait()
        part_s[:, k * chunk : (k + 1) * chunk] = jnp.dot(
            attn, weight[:, k * chunk : (k + 1) * chunk], preferred_element_type=jnp.float32
        )
    per = out_ref.shape[1]
    for k in range(out_ref.shape[0]):
        out_ref[k] = part_s[k * per : (k + 1) * per, :].astype(jnp.bfloat16)
    store = pltpu.make_async_copy(out_ref, out_hbm, small_sem.at[0])
    store.start()
    store.wait()


def attend(query, incoming_key, new_value, key_cache, value_cache, cache_len, out_weight, nz):
    slot_dev = query.shape[0]
    lines = slot_dev * (query.shape[1] // HEAD_DIM)
    hbm = pl.BlockSpec(memory_space=pltpu.HBM)
    return pl.pallas_call(
        attend_kernel,
        in_specs=[pl.BlockSpec(memory_space=pltpu.SMEM), *[hbm] * 6],
        out_specs=hbm,
        out_shape=jax.ShapeDtypeStruct((nz, slot_dev // nz, D), jnp.bfloat16),
        scratch_shapes=[
            pltpu.VMEM(key_cache.shape, jnp.bfloat16),
            pltpu.VMEM(value_cache.shape, jnp.bfloat16),
            pltpu.VMEM(out_weight.shape, jnp.bfloat16),
            pltpu.VMEM(query.shape, jnp.bfloat16),
            pltpu.VMEM(incoming_key.shape, jnp.bfloat16),
            pltpu.VMEM(new_value.shape, jnp.bfloat16),
            pltpu.VMEM((nz, slot_dev // nz, D), jnp.bfloat16),
            *[pltpu.VMEM((lines, HEAD_DIM), jnp.float32)] * 3,
            pltpu.VMEM((lines, key_cache.shape[1]), jnp.float32),
            pltpu.VMEM((lines, HEAD_DIM), jnp.float32),
            pltpu.VMEM((slot_dev, D), jnp.float32),
            pltpu.SemaphoreType.DMA((4,)),
            pltpu.SemaphoreType.DMA((4,)),
            pltpu.SemaphoreType.DMA((4,)),
            pltpu.SemaphoreType.DMA((3,)),
        ],
        compiler_params=params(61),
        cost_estimate=pl.CostEstimate(flops=2_000_000_000, bytes_accessed=9_000_000, transcendentals=20_000),
        name="attend",
    )(cache_len, query, incoming_key, new_value, key_cache, value_cache, out_weight)


def exchange(blocks, axes):
    return lax.all_to_all(blocks, axes, 0, 0, tiled=True)


def other_core(value):
    return lax.ppermute(value, "dp_2", [(0, 1), (1, 0)])


def inverse_rms(rows):
    return lax.rsqrt(jnp.mean(rows * rows, axis=-1, keepdims=True) + 1e-06)


def product(rows, slots):
    return lax.dot_general(
        rows, slots, (((1,), (1,)), ((), ())), preferred_element_type=jnp.float32
    )


def in_vmem(count):
    return [pl.BlockSpec(memory_space=pltpu.VMEM)] * count


def params(mib):
    return pltpu.CompilerParams(vmem_limit_bytes=mib * 1024 * 1024)


def mix_kernel(pieces_ref, residual_ref, gain_ref, out_ref):
    nz, per, _ = pieces_ref.shape
    z = lax.axis_index("tensor")
    proj = pieces_ref[0].astype(jnp.float32)
    for k in range(1, nz):
        proj = proj + pieces_ref[k].astype(jnp.float32)
    post = proj * inverse_rms(proj) * gain_ref[...].reshape(1, D)
    residual = residual_ref[...].astype(jnp.float32)
    row = lax.broadcasted_iota(jnp.int32, (residual.shape[0], 1), 0)
    picked = [
        jnp.sum(jnp.where(row == z * per + k, residual, 0.0), axis=0, keepdims=True)
        for k in range(per)
    ]
    mix = (jnp.concatenate(picked, axis=0) + post).astype(jnp.bfloat16)
    for k in range(nz):
        out_ref[k] = mix


def mix_rows(pieces, residual, gain):
    return pl.pallas_call(
        mix_kernel,
        in_specs=in_vmem(3),
        out_specs=in_vmem(1)[0],
        out_shape=jax.ShapeDtypeStruct(pieces.shape, jnp.bfloat16),
        compiler_params=params(4),
        name="mix_rows",
    )(pieces, residual, gain)


def as_column(line):
    size = line.shape[1]
    row = lax.broadcasted_iota(jnp.int32, (size, size), 0)
    lane = lax.broadcasted_iota(jnp.int32, (size, size), 1)
    return jnp.sum(jnp.where(row == lane, line, 0), axis=1, keepdims=True)


def hidden_kernel(
    mix_ref, gain_ref, sampled_ref, flag_ref, other_ref, turn_ref, last_ref, slice_ref, rows
):
    nz, per, _ = mix_ref.shape
    slot_dev, width = slice_ref.shape
    third = D // 3
    z = lax.axis_index("tensor")
    for k in range(nz):
        rows[k * per : (k + 1) * per, :] = mix_ref[k].astype(jnp.float32)
    mixed = rows[...]
    hidden = mixed * inverse_rms(mixed) * gain_ref[...].reshape(1, D)
    turn = jnp.where(z % 2 == 0, hidden[:, :third], hidden[:, third : 2 * third])
    turn = turn.astype(jnp.bfloat16)
    last = hidden[:, 2 * third :].astype(jnp.bfloat16)
    sampled = sampled_ref[...]
    freed = (flag_ref[...] == 1).astype(jnp.int32)
    count = jnp.sum((other_ref[...] == 1).astype(jnp.int32), axis=1, keepdims=True)
    values = [sampled & 63, (sampled >> 6) & 63, sampled >> 12, freed]
    lane = lax.broadcasted_iota(jnp.int32, (slot_dev, META), 1)
    notes = jnp.where(lane == 4, count, 0)
    for k, value in enumerate(values):
        notes = jnp.where(lane == k, as_column(value), notes)
    notes = notes.astype(jnp.float32).astype(jnp.bfloat16)
    for k in range(turn_ref.shape[0]):
        turn_ref[k] = turn
        last_ref[k, :, :third] = last
        last_ref[k, :, third:] = notes
    for k in range(nz):

        @pl.when(z == k)
        def _():
            slice_ref[...] = rows[:, k * width : (k + 1) * width].astype(jnp.bfloat16)


def hidden_blocks(mix, gain, sampled, flag, other_flag, planes):
    slot_dev = mix.shape[0] * mix.shape[1]
    width = D // mix.shape[0]
    return pl.pallas_call(
        hidden_kernel,
        in_specs=in_vmem(5),
        out_specs=in_vmem(3),
        out_shape=[
            jax.ShapeDtypeStruct((planes, slot_dev, D // 3), jnp.bfloat16),
            jax.ShapeDtypeStruct((planes, slot_dev, D // 3 + META), jnp.bfloat16),
            jax.ShapeDtypeStruct((slot_dev, width), jnp.bfloat16),
        ],
        scratch_shapes=[pltpu.VMEM((slot_dev, D), jnp.float32)],
        compiler_params=params(8),
        name="hidden_blocks",
    )(mix, gain, sampled, flag, other_flag)


def vocab_kernel(
    turn_ref, before_ref, after_ref, last_ref, notes_ref, own_ref, other_ref, flag_ref,
    pair_ref, rank_ref, total_ref, every,
):
    slots = turn_ref.shape[0]
    per_device = own_ref.shape[0]
    third = D // 3
    slot_dev = flag_ref.shape[1]
    planes = slots // slot_dev
    nz = pair_ref.shape[0] // planes
    z = lax.axis_index("tensor")
    core = lax.axis_index("dp_2")
    plane = lax.axis_index("dp_0") * lax.axis_size("dp_1") + lax.axis_index("dp_1")
    for parity in range(2):

        @pl.when(z % 2 == parity)
        def _():
            mine, theirs = parity * third, (1 - parity) * third
            every[:, mine : mine + third] = turn_ref[...]
            every[:, theirs : theirs + third // 2] = before_ref[...]
            every[:, theirs + third // 2 : theirs + third] = after_ref[...]

    every[:, 2 * third :] = last_ref[:, :third]
    lane = lax.broadcasted_iota(jnp.int32, (16, META), 1)
    row = lax.broadcasted_iota(jnp.int32, (16, META), 0)
    digit = jnp.where(lane == 0, 1.0, jnp.where(lane == 1, 64.0, jnp.where(lane == 2, 4096.0, 0.0)))
    pick = jnp.where(row == 0, digit, jnp.where(lane == row + 2, 1.0, 0.0))
    notes = product(pick.astype(jnp.bfloat16), notes_ref[...])
    ids = notes[0:1, :].astype(jnp.int32)
    line = lax.broadcasted_iota(jnp.int32, (per_device, slots), 0)
    tops, sums = [], []
    picked = jnp.zeros((1, slots), jnp.float32)
    for rows_ref, holder in ((own_ref, core), (other_ref, 1 - core)):
        begin = ((plane * 2 + holder) * nz + z) * per_device
        logits = product(rows_ref[...], every[...])
        picked = picked + jnp.sum(jnp.where(line == ids - begin, logits, 0.0), axis=0, keepdims=True)
        top = jnp.max(logits, axis=0, keepdims=True)
        tops.append(top)
        sums.append(jnp.sum(jnp.exp(logits - top), axis=0, keepdims=True))
    top = jnp.maximum(tops[0], tops[1])
    total = sums[0] * jnp.exp(tops[0] - top) + sums[1] * jnp.exp(tops[1] - top)
    entropy = top + jnp.log(total)
    for k in range(planes):
        for part, value in ((0, entropy), (1, picked)):
            pair_ref[k * nz : (k + 1) * nz, part * slot_dev : (part + 1) * slot_dev] = (
                jnp.broadcast_to(value[:, k * slot_dev : (k + 1) * slot_dev], (nz, slot_dev))
            )

    slot = lax.broadcasted_iota(jnp.int32, (1, slots), 1)
    flags = notes[1:2, :]
    counts = jnp.where(slot % slot_dev == 0, notes[2:3, :], 0.0)
    both = flags + counts
    total_ref[...] = jnp.sum(both, axis=1, keepdims=True).astype(jnp.int32)
    before = jnp.sum(jnp.where(slot // slot_dev < plane, both, 0.0), axis=1, keepdims=True)
    partner = jnp.sum(jnp.where(slot == plane * slot_dev, counts, 0.0), axis=1, keepdims=True)
    before = (before + jnp.where(core == 1, partner, 0.0)).astype(jnp.int32)
    freed = (flag_ref[...] == 1).astype(jnp.int32)
    below = lax.broadcasted_iota(jnp.int32, (slot_dev, slot_dev), 0)
    place = lax.broadcasted_iota(jnp.int32, (slot_dev, slot_dev), 1)
    ahead = jnp.sum(jnp.where(below < place, as_column(freed), 0), axis=0, keepdims=True)
    rank_ref[...] = jnp.where(freed == 1, ahead + before, -1)


def vocab_stats(turn, before, after, last, notes, own, other, flag, nz):
    slots = turn.shape[0]
    rows = own.shape[0]
    slot_dev = flag.shape[1]
    return pl.pallas_call(
        vocab_kernel,
        in_specs=in_vmem(8),
        out_specs=in_vmem(3),
        out_shape=[
            jax.ShapeDtypeStruct((slots // slot_dev * nz, 2 * slot_dev), jnp.float32),
            jax.ShapeDtypeStruct((1, slot_dev), jnp.int32),
            jax.ShapeDtypeStruct((1, 1), jnp.int32),
        ],
        scratch_shapes=[pltpu.VMEM((slots, D), jnp.bfloat16)],
        compiler_params=params(20),
        cost_estimate=pl.CostEstimate(
            flops=4 * rows * slots * D, bytes_accessed=4 * rows * D, transcendentals=2 * rows * slots
        ),
        name="vocab_stats",
    )(turn, before, after, last, notes, own, other, flag)


def on_device(
    query,
    incoming_key,
    new_value,
    key_cache,
    value_cache,
    cache_len,
    out_weight,
    residual,
    post_gain,
    final_gain,
    vocab_weight,
    sampled,
    stop_flag,
):
    slot_dev = query.shape[0]
    nz = lax.axis_size("tensor")
    planes = lax.axis_size(PLANE)
    other_flag = other_core(stop_flag)
    blocks = attend(
        query, incoming_key, new_value, key_cache, value_cache, cache_len, out_weight, nz
    )
    flag, sampled_line = stop_flag.reshape(1, slot_dev), sampled.reshape(1, slot_dev)
    blocks, vocab_weight, other_flag, flag, sampled_line = lax.optimization_barrier(
        (blocks, vocab_weight, other_flag, flag, sampled_line)
    )
    vocab_other = other_core(vocab_weight)
    pieces = exchange(blocks, "tensor")
    mix = exchange(mix_rows(pieces, residual, post_gain), "tensor")
    mix, vocab_other = lax.optimization_barrier((mix, vocab_other))
    vocab_own = other_core(vocab_other)
    turn, last, new_residual = hidden_blocks(
        mix,
        final_gain,
        sampled_line,
        flag,
        other_flag.reshape(1, slot_dev),
        planes,
    )
    slots = planes * slot_dev
    half = D // 6
    turn = exchange(turn, PLANE).reshape(slots, D // 3)
    left, right, turn, last = lax.optimization_barrier((turn[:, :half], turn[:, half:], turn, last))
    before = lax.ppermute(left, "tensor", [(k, (k + 1) % nz) for k in range(nz)])
    after = lax.ppermute(right, "tensor", [((k + 1) % nz, k) for k in range(nz)])
    last = exchange(last, PLANE).reshape(slots, D // 3 + META)
    notes = last[:, D // 3 :]
    pair, rank, released = vocab_stats(
        turn, before, after, last, notes, vocab_own, vocab_other, flag, nz
    )
    gathered = exchange(pair, CHIPS)
    parts = gathered[:, :slot_dev]
    highest = jnp.max(parts, axis=0)
    overall = jnp.log(jnp.sum(jnp.exp(parts - highest[None]), axis=0)) + highest
    token_logprob = jnp.sum(gathered[:, slot_dev:], axis=0) - overall
    return (new_residual, token_logprob, rank.reshape(slot_dev), released.reshape(()))


def solution(mesh):
    split = Mesh(
        mesh.devices.reshape(4, 4, 2, mesh.shape["tensor"]), ("dp_0", "dp_1", "dp_2", "tensor")
    )
    in_specs = (
        P(DP, "tensor"),
        P(DP, "tensor"),
        P(DP, "tensor"),
        P(DP, None, "tensor"),
        P(DP, None, "tensor"),
        P(DP),
        P("tensor", None),
        P(DP, None),
        P(),
        P(),
        P(DP_TENSOR, None),
        P(DP),
        P(DP),
    )
    out_specs = (P(DP, "tensor"), P(DP), P(DP), P())
    return jax.shard_map(
        on_device, mesh=split, in_specs=in_specs, out_specs=out_specs, check_vma=False
    )
```

```python
import jax
import jax.numpy as jnp
from jax import lax
from jax.experimental import pallas as pl
from jax.experimental.pallas import tpu as pltpu
from jax.sharding import Mesh
from jax.sharding import PartitionSpec as P

D = 4608
HEADS = 32
KV_HEADS = 16
HEAD_DIM = 128
DP = ("dp_0", "dp_1", "dp_2")
DP_TENSOR = ("dp_0", "dp_1", "dp_2", "tensor")
PLANE = ("dp_0", "dp_1")
CHIPS = ("dp_0", "dp_1", "tensor")
META = 128


def attend_kernel(
    len_ref, query_hbm, key_hbm, value_hbm, keys_hbm, values_hbm, weight_hbm, out_hbm,
    keys, values, weight, query_ref, key_ref, value_ref, out_ref,
    query_s, key_s, value_s, score_s, attn_s, key_sem, value_sem, weight_sem, small_sem, out_sem,
):
    slot_dev = keys.shape[0]
    positions = keys.shape[1]
    group = HEADS // KV_HEADS
    heads = query_ref.shape[1] // HEAD_DIM
    kv_local = heads // group
    batch = slot_dev // key_sem.shape[0]
    chunk = D // weight_sem.shape[0]
    loads = {}
    smalls = ((query_hbm, query_ref), (key_hbm, key_ref), (value_hbm, value_ref))
    for k, (source, target) in enumerate(smalls):
        loads["s", k] = pltpu.make_async_copy(source, target, small_sem.at[k])
        loads["s", k].start()
    for name, source, target, sem in (("k", keys_hbm, keys, key_sem), ("v", values_hbm, values, value_sem)):
        for k in range(sem.shape[0]):
            part = pl.ds(k * batch, batch)
            loads[name, k] = pltpu.make_async_copy(source.at[part], target.at[part], sem.at[k])
            loads[name, k].start()
    for k in range(weight_sem.shape[0]):
        part = pl.ds(k * chunk, chunk)
        loads["w", k] = pltpu.make_async_copy(
            weight_hbm.at[:, part], weight.at[:, part], weight_sem.at[k]
        )

    for k in range(len(smalls)):
        loads["s", k].wait()
    for h in range(heads):
        at = pl.ds(h, slot_dev, stride=heads)
        kv = h // group * HEAD_DIM
        query_s[at, :] = query_ref[:, h * HEAD_DIM : (h + 1) * HEAD_DIM].astype(jnp.float32)
        key_s[at, :] = key_ref[:, kv : kv + HEAD_DIM].astype(jnp.float32)
        value_s[at, :] = value_ref[:, kv : kv + HEAD_DIM].astype(jnp.float32)

    lines = 8
    pair = lines // heads
    row = lax.broadcasted_iota(jnp.int32, (lines, 1), 0)
    kind = row % heads // group

    def per_slot(rows, source, first, contract):
        found = None
        for k in range(pair):
            part = lax.dot_general(
                rows, source[first + k], (((1,), (contract,)), ((), ())), preferred_element_type=jnp.float32
            )
            found = part if found is None else jnp.where(row >= k * heads, part, found)
        return found

    for i in range(slot_dev // pair):
        if i * pair % batch == 0:
            loads["k", i * pair // batch].wait()
        rows = query_s[i * lines : (i + 1) * lines, :]
        spread = [jnp.where(kind == k, rows, 0.0) for k in range(kv_local)]
        spread = jnp.concatenate(spread, axis=1).astype(jnp.bfloat16)
        score_s[i * lines : (i + 1) * lines, :] = per_slot(spread, keys, i * pair, 1)
        if (i + 1) * pair % batch == 0:
            loads["w", i * pair // batch].start()

    total_rows = slot_dev * heads
    owner = lax.broadcasted_iota(jnp.int32, (total_rows, 1), 0) // heads
    length = jnp.zeros((total_rows, 1), jnp.int32)
    for k in range(slot_dev):
        length = jnp.where(owner == k, len_ref[k], length)
    valid = lax.broadcasted_iota(jnp.int32, (total_rows, positions), 1) < length
    scores = jnp.where(valid, score_s[...] / 12.0, -1e30)
    own = jnp.sum(query_s[...] * key_s[...], axis=1, keepdims=True) / 12.0
    top = jnp.maximum(jnp.max(scores, axis=1, keepdims=True), own)
    expo = jnp.where(valid, jnp.exp(scores - top), 0.0)
    own_exp = jnp.exp(own - top)
    total = jnp.sum(expo, axis=1, keepdims=True) + own_exp
    score_s[...] = expo / total
    own_weight = (own_exp / total).astype(jnp.bfloat16).astype(jnp.float32)

    for i in range(slot_dev // pair):
        if i * pair % batch == 0:
            loads["v", i * pair // batch].wait()
        rows = score_s[i * lines : (i + 1) * lines, :].astype(jnp.bfloat16)
        mixed = per_slot(rows, values, i * pair, 0)
        found = mixed[:, :HEAD_DIM]
        for k in range(1, kv_local):
            found = jnp.where(kind == k, mixed[:, k * HEAD_DIM : (k + 1) * HEAD_DIM], found)
        attn_s[i * lines : (i + 1) * lines, :] = found
    attn_s[...] += own_weight * value_s[...]
    attn = [attn_s[pl.ds(h, slot_dev, stride=heads), :] for h in range(heads)]
    attn = jnp.concatenate(attn, axis=1).astype(jnp.bfloat16)
    per = out_ref.shape[1]
    stores = []
    for k in range(weight_sem.shape[0]):
        loads["w", k].wait()
        columns = slice(k * chunk, (k + 1) * chunk)
        part = jnp.dot(attn, weight[:, columns], preferred_element_type=jnp.float32)
        for p in range(out_ref.shape[0]):
            out_ref[p, :, columns] = part[p * per : (p + 1) * per, :].astype(jnp.bfloat16)
        where = pl.ds(k * chunk, chunk)
        stores.append(
            pltpu.make_async_copy(out_ref.at[:, :, where], out_hbm.at[:, :, where], out_sem.at[k])
        )
        stores[-1].start()
    for store in stores:
        store.wait()


def attend(query, incoming_key, new_value, key_cache, value_cache, cache_len, out_weight, nz):
    slot_dev = query.shape[0]
    lines = slot_dev * (query.shape[1] // HEAD_DIM)
    hbm = pl.BlockSpec(memory_space=pltpu.HBM)
    return pl.pallas_call(
        attend_kernel,
        in_specs=[pl.BlockSpec(memory_space=pltpu.SMEM), *[hbm] * 6],
        out_specs=hbm,
        out_shape=jax.ShapeDtypeStruct((nz, slot_dev // nz, D), jnp.bfloat16),
        scratch_shapes=[
            pltpu.VMEM(key_cache.shape, jnp.bfloat16),
            pltpu.VMEM(value_cache.shape, jnp.bfloat16),
            pltpu.VMEM(out_weight.shape, jnp.bfloat16),
            pltpu.VMEM(query.shape, jnp.bfloat16),
            pltpu.VMEM(incoming_key.shape, jnp.bfloat16),
            pltpu.VMEM(new_value.shape, jnp.bfloat16),
            pltpu.VMEM((nz, slot_dev // nz, D), jnp.bfloat16),
            *[pltpu.VMEM((lines, HEAD_DIM), jnp.float32)] * 3,
            pltpu.VMEM((lines, key_cache.shape[1]), jnp.float32),
            pltpu.VMEM((lines, HEAD_DIM), jnp.float32),
            pltpu.SemaphoreType.DMA((4,)),
            pltpu.SemaphoreType.DMA((4,)),
            pltpu.SemaphoreType.DMA((4,)),
            pltpu.SemaphoreType.DMA((3,)),
            pltpu.SemaphoreType.DMA((4,)),
        ],
        compiler_params=params(61),
        cost_estimate=pl.CostEstimate(flops=2_000_000_000, bytes_accessed=9_000_000, transcendentals=20_000),
        name="attend",
    )(cache_len, query, incoming_key, new_value, key_cache, value_cache, out_weight)


def exchange(blocks, axes):
    return lax.all_to_all(blocks, axes, 0, 0, tiled=True)


def other_core(value):
    return lax.ppermute(value, "dp_2", [(0, 1), (1, 0)])


def inverse_rms(rows):
    return lax.rsqrt(jnp.mean(rows * rows, axis=-1, keepdims=True) + 1e-06)


def product(rows, slots):
    return lax.dot_general(
        rows, slots, (((1,), (1,)), ((), ())), preferred_element_type=jnp.float32
    )


def in_vmem(count):
    return [pl.BlockSpec(memory_space=pltpu.VMEM)] * count


def params(mib):
    return pltpu.CompilerParams(vmem_limit_bytes=mib * 1024 * 1024)


def mix_kernel(pieces_ref, residual_ref, gain_ref, out_ref):
    nz, per, _ = pieces_ref.shape
    z = lax.axis_index("tensor")
    proj = pieces_ref[0].astype(jnp.float32)
    for k in range(1, nz):
        proj = proj + pieces_ref[k].astype(jnp.float32)
    post = proj * inverse_rms(proj) * gain_ref[...].reshape(1, D)
    residual = residual_ref[...].astype(jnp.float32)
    row = lax.broadcasted_iota(jnp.int32, (residual.shape[0], 1), 0)
    picked = [
        jnp.sum(jnp.where(row == z * per + k, residual, 0.0), axis=0, keepdims=True)
        for k in range(per)
    ]
    mix = (jnp.concatenate(picked, axis=0) + post).astype(jnp.bfloat16)
    for k in range(nz):
        out_ref[k] = mix


def mix_rows(pieces, residual, gain):
    return pl.pallas_call(
        mix_kernel,
        in_specs=in_vmem(3),
        out_specs=in_vmem(1)[0],
        out_shape=jax.ShapeDtypeStruct(pieces.shape, jnp.bfloat16),
        compiler_params=params(4),
        name="mix_rows",
    )(pieces, residual, gain)


def as_column(line):
    size = line.shape[1]
    row = lax.broadcasted_iota(jnp.int32, (size, size), 0)
    lane = lax.broadcasted_iota(jnp.int32, (size, size), 1)
    return jnp.sum(jnp.where(row == lane, line, 0), axis=1, keepdims=True)


def hidden_kernel(mix_ref, gain_ref, sampled_ref, flag_ref, other_ref, block_ref, slice_ref, rows):
    nz, per, _ = mix_ref.shape
    slot_dev, width = slice_ref.shape
    z = lax.axis_index("tensor")
    for k in range(nz):
        rows[k * per : (k + 1) * per, :] = mix_ref[k].astype(jnp.float32)
    mixed = rows[...]
    hidden = (mixed * inverse_rms(mixed) * gain_ref[...].reshape(1, D)).astype(jnp.bfloat16)
    sampled = sampled_ref[...]
    freed = (flag_ref[...] == 1).astype(jnp.int32)
    count = jnp.sum((other_ref[...] == 1).astype(jnp.int32), axis=1, keepdims=True)
    values = [sampled & 63, (sampled >> 6) & 63, sampled >> 12, freed]
    lane = lax.broadcasted_iota(jnp.int32, (slot_dev, META), 1)
    notes = jnp.where(lane == 4, count, 0)
    for k, value in enumerate(values):
        notes = jnp.where(lane == k, as_column(value), notes)
    notes = notes.astype(jnp.float32).astype(jnp.bfloat16)
    for k in range(block_ref.shape[0]):
        block_ref[k, :, :D] = hidden
        block_ref[k, :, D:] = notes
    for k in range(nz):

        @pl.when(z == k)
        def _():
            slice_ref[...] = rows[:, k * width : (k + 1) * width].astype(jnp.bfloat16)


def hidden_blocks(mix, gain, sampled, flag, other_flag, planes):
    slot_dev = mix.shape[0] * mix.shape[1]
    width = D // mix.shape[0]
    return pl.pallas_call(
        hidden_kernel,
        in_specs=in_vmem(5),
        out_specs=in_vmem(2),
        out_shape=[
            jax.ShapeDtypeStruct((planes, slot_dev, D + META), jnp.bfloat16),
            jax.ShapeDtypeStruct((slot_dev, width), jnp.bfloat16),
        ],
        scratch_shapes=[pltpu.VMEM((slot_dev, D), jnp.float32)],
        compiler_params=params(8),
        name="hidden_blocks",
    )(mix, gain, sampled, flag, other_flag)


def vocab_kernel(
    every_ref, own_ref, other_ref, flag_ref, pair_ref, rank_ref, total_ref
):
    slots = every_ref.shape[0]
    per_device = own_ref.shape[0]
    slot_dev = flag_ref.shape[1]
    planes = slots // slot_dev
    nz = pair_ref.shape[0] // planes
    z = lax.axis_index("tensor")
    core = lax.axis_index("dp_2")
    plane = lax.axis_index("dp_0") * lax.axis_size("dp_1") + lax.axis_index("dp_1")
    lane = lax.broadcasted_iota(jnp.int32, (16, META), 1)
    row = lax.broadcasted_iota(jnp.int32, (16, META), 0)
    digit = jnp.where(lane == 0, 1.0, jnp.where(lane == 1, 64.0, jnp.where(lane == 2, 4096.0, 0.0)))
    pick = jnp.where(row == 0, digit, jnp.where(lane == row + 2, 1.0, 0.0))
    notes = product(pick.astype(jnp.bfloat16), every_ref[:, D:])
    ids = notes[0:1, :].astype(jnp.int32)
    line = lax.broadcasted_iota(jnp.int32, (per_device, slots), 0)
    tops, sums = [], []
    picked = jnp.zeros((1, slots), jnp.float32)
    for rows_ref, holder in ((own_ref, core), (other_ref, 1 - core)):
        begin = ((plane * 2 + holder) * nz + z) * per_device
        logits = product(rows_ref[...], every_ref[:, :D])
        picked = picked + jnp.sum(jnp.where(line == ids - begin, logits, 0.0), axis=0, keepdims=True)
        top = jnp.max(logits, axis=0, keepdims=True)
        tops.append(top)
        sums.append(jnp.sum(jnp.exp(logits - top), axis=0, keepdims=True))
    top = jnp.maximum(tops[0], tops[1])
    total = sums[0] * jnp.exp(tops[0] - top) + sums[1] * jnp.exp(tops[1] - top)
    entropy = top + jnp.log(total)
    for k in range(planes):
        for part, value in ((0, entropy), (1, picked)):
            pair_ref[k * nz : (k + 1) * nz, part * slot_dev : (part + 1) * slot_dev] = (
                jnp.broadcast_to(value[:, k * slot_dev : (k + 1) * slot_dev], (nz, slot_dev))
            )

    slot = lax.broadcasted_iota(jnp.int32, (1, slots), 1)
    flags = notes[1:2, :]
    counts = jnp.where(slot % slot_dev == 0, notes[2:3, :], 0.0)
    both = flags + counts
    total_ref[...] = jnp.sum(both, axis=1, keepdims=True).astype(jnp.int32)
    before = jnp.sum(jnp.where(slot // slot_dev < plane, both, 0.0), axis=1, keepdims=True)
    partner = jnp.sum(jnp.where(slot == plane * slot_dev, counts, 0.0), axis=1, keepdims=True)
    before = (before + jnp.where(core == 1, partner, 0.0)).astype(jnp.int32)
    freed = (flag_ref[...] == 1).astype(jnp.int32)
    below = lax.broadcasted_iota(jnp.int32, (slot_dev, slot_dev), 0)
    place = lax.broadcasted_iota(jnp.int32, (slot_dev, slot_dev), 1)
    ahead = jnp.sum(jnp.where(below < place, as_column(freed), 0), axis=0, keepdims=True)
    rank_ref[...] = jnp.where(freed == 1, ahead + before, -1)


def vocab_stats(every, own, other, flag, nz):
    slots = every.shape[0]
    rows = own.shape[0]
    slot_dev = flag.shape[1]
    return pl.pallas_call(
        vocab_kernel,
        in_specs=in_vmem(4),
        out_specs=in_vmem(3),
        out_shape=[
            jax.ShapeDtypeStruct((slots // slot_dev * nz, 2 * slot_dev), jnp.float32),
            jax.ShapeDtypeStruct((1, slot_dev), jnp.int32),
            jax.ShapeDtypeStruct((1, 1), jnp.int32),
        ],
        compiler_params=params(20),
        cost_estimate=pl.CostEstimate(
            flops=4 * rows * slots * D, bytes_accessed=4 * rows * D, transcendentals=2 * rows * slots
        ),
        name="vocab_stats",
    )(every, own, other, flag)


def on_device(
    query,
    incoming_key,
    new_value,
    key_cache,
    value_cache,
    cache_len,
    out_weight,
    residual,
    post_gain,
    final_gain,
    vocab_weight,
    sampled,
    stop_flag,
):
    slot_dev = query.shape[0]
    nz = lax.axis_size("tensor")
    planes = lax.axis_size(PLANE)
    other_flag = other_core(stop_flag)

    blocks = attend(
        query, incoming_key, new_value, key_cache, value_cache, cache_len, out_weight, nz
    )
    flag, sampled_line = stop_flag.reshape(1, slot_dev), sampled.reshape(1, slot_dev)
    blocks, vocab_weight, other_flag, flag, sampled_line = lax.optimization_barrier(
        (blocks, vocab_weight, other_flag, flag, sampled_line)
    )
    vocab_other = other_core(vocab_weight)
    pieces = exchange(blocks, "tensor")
    mix = exchange(mix_rows(pieces, residual, post_gain), "tensor")
    hidden, new_residual = hidden_blocks(
        mix,
        final_gain,
        sampled_line,
        flag,
        other_flag.reshape(1, slot_dev),
        planes,
    )
    every = exchange(hidden, PLANE).reshape(planes * slot_dev, D + META)
    pair, rank, released = vocab_stats(every, vocab_weight, vocab_other, flag, nz)
    gathered = exchange(pair, CHIPS)
    parts = gathered[:, :slot_dev]
    highest = jnp.max(parts, axis=0)
    overall = jnp.log(jnp.sum(jnp.exp(parts - highest[None]), axis=0)) + highest
    token_logprob = jnp.sum(gathered[:, slot_dev:], axis=0) - overall
    return (new_residual, token_logprob, rank.reshape(slot_dev), released.reshape(()))


def solution(mesh):
    split = Mesh(
        mesh.devices.reshape(4, 4, 2, mesh.shape["tensor"]), ("dp_0", "dp_1", "dp_2", "tensor")
    )
    in_specs = (
        P(DP, "tensor"),
        P(DP, "tensor"),
        P(DP, "tensor"),
        P(DP, None, "tensor"),
        P(DP, None, "tensor"),
        P(DP),
        P("tensor", None),
        P(DP, None),
        P(),
        P(),
        P(DP_TENSOR, None),
        P(DP),
        P(DP),
    )
    out_specs = (P(DP, "tensor"), P(DP), P(DP), P())
    return jax.shard_map(
        on_device, mesh=split, in_specs=in_specs, out_specs=out_specs, check_vma=False
    )
```

```python
import jax
import jax.numpy as jnp
from jax import lax
from jax.experimental import pallas as pl
from jax.experimental.pallas import tpu as pltpu
from jax.sharding import Mesh
from jax.sharding import PartitionSpec as P

D = 4608
HEADS = 32
KV_HEADS = 16
HEAD_DIM = 128
DP = ("dp_0", "dp_1", "dp_2")
DP_TENSOR = ("dp_0", "dp_1", "dp_2", "tensor")
PLANE = ("dp_0", "dp_1")
CHIPS = ("dp_0", "dp_1", "tensor")
META = 128


def attend_kernel(
    len_ref, query_hbm, key_hbm, value_hbm, keys_hbm, values_hbm, weight_hbm, out_hbm,
    keys, values, weight, query_ref, key_ref, value_ref, out_ref,
    query_s, key_s, value_s, score_s, attn_s, key_sem, value_sem, weight_sem, small_sem, out_sem,
):
    slot_dev = keys.shape[0]
    positions = keys.shape[1]
    group = HEADS // KV_HEADS
    heads = query_ref.shape[1] // HEAD_DIM
    kv_local = heads // group
    batch = slot_dev // key_sem.shape[0]
    chunk = D // weight_sem.shape[0]
    pace = slot_dev // weight_sem.shape[0]
    loads = {}
    smalls = ((query_hbm, query_ref), (key_hbm, key_ref), (value_hbm, value_ref))
    for k, (source, target) in enumerate(smalls):
        loads["s", k] = pltpu.make_async_copy(source, target, small_sem.at[k])
        loads["s", k].start()
    for name, source, target, sem in (("k", keys_hbm, keys, key_sem), ("v", values_hbm, values, value_sem)):
        for k in range(sem.shape[0]):
            part = pl.ds(k * batch, batch)
            loads[name, k] = pltpu.make_async_copy(source.at[part], target.at[part], sem.at[k])
            loads[name, k].start()
    for k in range(weight_sem.shape[0]):
        part = pl.ds(k * chunk, chunk)
        loads["w", k] = pltpu.make_async_copy(
            weight_hbm.at[:, part], weight.at[:, part], weight_sem.at[k]
        )

    for k in range(len(smalls)):
        loads["s", k].wait()
    for h in range(heads):
        at = pl.ds(h, slot_dev, stride=heads)
        kv = h // group * HEAD_DIM
        query_s[at, :] = query_ref[:, h * HEAD_DIM : (h + 1) * HEAD_DIM].astype(jnp.float32)
        key_s[at, :] = key_ref[:, kv : kv + HEAD_DIM].astype(jnp.float32)
        value_s[at, :] = value_ref[:, kv : kv + HEAD_DIM].astype(jnp.float32)

    lines = 8
    pair = lines // heads
    row = lax.broadcasted_iota(jnp.int32, (lines, 1), 0)
    kind = row % heads // group

    def per_slot(rows, source, first, contract):
        found = None
        for k in range(pair):
            part = lax.dot_general(
                rows, source[first + k], (((1,), (contract,)), ((), ())), preferred_element_type=jnp.float32
            )
            found = part if found is None else jnp.where(row >= k * heads, part, found)
        return found

    for i in range(slot_dev // pair):
        if i * pair % batch == 0:
            loads["k", i * pair // batch].wait()
        rows = query_s[i * lines : (i + 1) * lines, :]
        spread = [jnp.where(kind == k, rows, 0.0) for k in range(kv_local)]
        spread = jnp.concatenate(spread, axis=1).astype(jnp.bfloat16)
        score_s[i * lines : (i + 1) * lines, :] = per_slot(spread, keys, i * pair, 1)
        if (i + 1) * pair % pace == 0:
            loads["w", i * pair // pace].start()

    total_rows = slot_dev * heads
    owner = lax.broadcasted_iota(jnp.int32, (total_rows, 1), 0) // heads
    length = jnp.zeros((total_rows, 1), jnp.int32)
    for k in range(slot_dev):
        length = jnp.where(owner == k, len_ref[k], length)
    valid = lax.broadcasted_iota(jnp.int32, (total_rows, positions), 1) < length
    scores = jnp.where(valid, score_s[...] / 12.0, -1e30)
    own = jnp.sum(query_s[...] * key_s[...], axis=1, keepdims=True) / 12.0
    top = jnp.maximum(jnp.max(scores, axis=1, keepdims=True), own)
    expo = jnp.where(valid, jnp.exp(scores - top), 0.0)
    own_exp = jnp.exp(own - top)
    total = jnp.sum(expo, axis=1, keepdims=True) + own_exp
    score_s[...] = expo / total
    own_weight = (own_exp / total).astype(jnp.bfloat16).astype(jnp.float32)

    for i in range(slot_dev // pair):
        if i * pair % batch == 0:
            loads["v", i * pair // batch].wait()
        rows = score_s[i * lines : (i + 1) * lines, :].astype(jnp.bfloat16)
        mixed = per_slot(rows, values, i * pair, 0)
        found = mixed[:, :HEAD_DIM]
        for k in range(1, kv_local):
            found = jnp.where(kind == k, mixed[:, k * HEAD_DIM : (k + 1) * HEAD_DIM], found)
        attn_s[i * lines : (i + 1) * lines, :] = found
    attn_s[...] += own_weight * value_s[...]
    attn = [attn_s[pl.ds(h, slot_dev, stride=heads), :] for h in range(heads)]
    attn = jnp.concatenate(attn, axis=1).astype(jnp.bfloat16)
    per = out_ref.shape[1]
    stores = []
    for k in range(weight_sem.shape[0]):
        loads["w", k].wait()
        columns = slice(k * chunk, (k + 1) * chunk)
        part = jnp.dot(attn, weight[:, columns], preferred_element_type=jnp.float32)
        for p in range(out_ref.shape[0]):
            out_ref[p, :, columns] = part[p * per : (p + 1) * per, :].astype(jnp.bfloat16)
        where = pl.ds(k * chunk, chunk)
        stores.append(
            pltpu.make_async_copy(out_ref.at[:, :, where], out_hbm.at[:, :, where], out_sem.at[k])
        )
        stores[-1].start()
    for store in stores:
        store.wait()


def attend(query, incoming_key, new_value, key_cache, value_cache, cache_len, out_weight, nz):
    slot_dev = query.shape[0]
    lines = slot_dev * (query.shape[1] // HEAD_DIM)
    hbm = pl.BlockSpec(memory_space=pltpu.HBM)
    return pl.pallas_call(
        attend_kernel,
        in_specs=[pl.BlockSpec(memory_space=pltpu.SMEM), *[hbm] * 6],
        out_specs=hbm,
        out_shape=jax.ShapeDtypeStruct((nz, slot_dev // nz, D), jnp.bfloat16),
        scratch_shapes=[
            pltpu.VMEM(key_cache.shape, jnp.bfloat16),
            pltpu.VMEM(value_cache.shape, jnp.bfloat16),
            pltpu.VMEM(out_weight.shape, jnp.bfloat16),
            pltpu.VMEM(query.shape, jnp.bfloat16),
            pltpu.VMEM(incoming_key.shape, jnp.bfloat16),
            pltpu.VMEM(new_value.shape, jnp.bfloat16),
            pltpu.VMEM((nz, slot_dev // nz, D), jnp.bfloat16),
            *[pltpu.VMEM((lines, HEAD_DIM), jnp.float32)] * 3,
            pltpu.VMEM((lines, key_cache.shape[1]), jnp.float32),
            pltpu.VMEM((lines, HEAD_DIM), jnp.float32),
            pltpu.SemaphoreType.DMA((8,)),
            pltpu.SemaphoreType.DMA((8,)),
            pltpu.SemaphoreType.DMA((4,)),
            pltpu.SemaphoreType.DMA((3,)),
            pltpu.SemaphoreType.DMA((4,)),
        ],
        compiler_params=params(61),
        cost_estimate=pl.CostEstimate(flops=2_000_000_000, bytes_accessed=9_000_000, transcendentals=20_000),
        name="attend",
    )(cache_len, query, incoming_key, new_value, key_cache, value_cache, out_weight)


def exchange(blocks, axes):
    return lax.all_to_all(blocks, axes, 0, 0, tiled=True)


def other_core(value):
    return lax.ppermute(value, "dp_2", [(0, 1), (1, 0)])


def inverse_rms(rows):
    return lax.rsqrt(jnp.mean(rows * rows, axis=-1, keepdims=True) + 1e-06)


def product(rows, slots):
    return lax.dot_general(
        rows, slots, (((1,), (1,)), ((), ())), preferred_element_type=jnp.float32
    )


def in_vmem(count):
    return [pl.BlockSpec(memory_space=pltpu.VMEM)] * count


def params(mib):
    return pltpu.CompilerParams(vmem_limit_bytes=mib * 1024 * 1024)


def mix_kernel(pieces_ref, residual_ref, gain_ref, out_ref):
    nz, per, _ = pieces_ref.shape
    z = lax.axis_index("tensor")
    proj = pieces_ref[0].astype(jnp.float32)
    for k in range(1, nz):
        proj = proj + pieces_ref[k].astype(jnp.float32)
    post = proj * inverse_rms(proj) * gain_ref[...].reshape(1, D)
    residual = residual_ref[...].astype(jnp.float32)
    row = lax.broadcasted_iota(jnp.int32, (residual.shape[0], 1), 0)
    picked = [
        jnp.sum(jnp.where(row == z * per + k, residual, 0.0), axis=0, keepdims=True)
        for k in range(per)
    ]
    mix = (jnp.concatenate(picked, axis=0) + post).astype(jnp.bfloat16)
    for k in range(nz):
        out_ref[k] = mix


def mix_rows(pieces, residual, gain):
    return pl.pallas_call(
        mix_kernel,
        in_specs=in_vmem(3),
        out_specs=in_vmem(1)[0],
        out_shape=jax.ShapeDtypeStruct(pieces.shape, jnp.bfloat16),
        compiler_params=params(4),
        name="mix_rows",
    )(pieces, residual, gain)


def as_column(line):
    size = line.shape[1]
    row = lax.broadcasted_iota(jnp.int32, (size, size), 0)
    lane = lax.broadcasted_iota(jnp.int32, (size, size), 1)
    return jnp.sum(jnp.where(row == lane, line, 0), axis=1, keepdims=True)


def hidden_kernel(mix_ref, gain_ref, sampled_ref, flag_ref, other_ref, block_ref, slice_ref, rows):
    nz, per, _ = mix_ref.shape
    slot_dev, width = slice_ref.shape
    z = lax.axis_index("tensor")
    for k in range(nz):
        rows[k * per : (k + 1) * per, :] = mix_ref[k].astype(jnp.float32)
    mixed = rows[...]
    hidden = (mixed * inverse_rms(mixed) * gain_ref[...].reshape(1, D)).astype(jnp.bfloat16)
    sampled = sampled_ref[...]
    freed = (flag_ref[...] == 1).astype(jnp.int32)
    count = jnp.sum((other_ref[...] == 1).astype(jnp.int32), axis=1, keepdims=True)
    values = [sampled & 63, (sampled >> 6) & 63, sampled >> 12, freed]
    lane = lax.broadcasted_iota(jnp.int32, (slot_dev, META), 1)
    notes = jnp.where(lane == 4, count, 0)
    for k, value in enumerate(values):
        notes = jnp.where(lane == k, as_column(value), notes)
    notes = notes.astype(jnp.float32).astype(jnp.bfloat16)
    for k in range(block_ref.shape[0]):
        block_ref[k, :, :D] = hidden
        block_ref[k, :, D:] = notes
    for k in range(nz):

        @pl.when(z == k)
        def _():
            slice_ref[...] = rows[:, k * width : (k + 1) * width].astype(jnp.bfloat16)


def hidden_blocks(mix, gain, sampled, flag, other_flag, planes):
    slot_dev = mix.shape[0] * mix.shape[1]
    width = D // mix.shape[0]
    return pl.pallas_call(
        hidden_kernel,
        in_specs=in_vmem(5),
        out_specs=in_vmem(2),
        out_shape=[
            jax.ShapeDtypeStruct((planes, slot_dev, D + META), jnp.bfloat16),
            jax.ShapeDtypeStruct((slot_dev, width), jnp.bfloat16),
        ],
        scratch_shapes=[pltpu.VMEM((slot_dev, D), jnp.float32)],
        compiler_params=params(8),
        name="hidden_blocks",
    )(mix, gain, sampled, flag, other_flag)


def vocab_kernel(
    every_ref, own_ref, other_ref, flag_ref, pair_ref, rank_ref, total_ref
):
    slots = every_ref.shape[0]
    per_device = own_ref.shape[0]
    slot_dev = flag_ref.shape[1]
    planes = slots // slot_dev
    nz = pair_ref.shape[0] // planes
    z = lax.axis_index("tensor")
    core = lax.axis_index("dp_2")
    plane = lax.axis_index("dp_0") * lax.axis_size("dp_1") + lax.axis_index("dp_1")
    lane = lax.broadcasted_iota(jnp.int32, (16, META), 1)
    row = lax.broadcasted_iota(jnp.int32, (16, META), 0)
    digit = jnp.where(lane == 0, 1.0, jnp.where(lane == 1, 64.0, jnp.where(lane == 2, 4096.0, 0.0)))
    pick = jnp.where(row == 0, digit, jnp.where(lane == row + 2, 1.0, 0.0))
    notes = product(pick.astype(jnp.bfloat16), every_ref[:, D:])
    ids = notes[0:1, :].astype(jnp.int32)
    line = lax.broadcasted_iota(jnp.int32, (per_device, slots), 0)
    tops, sums = [], []
    picked = jnp.zeros((1, slots), jnp.float32)
    for rows_ref, holder in ((own_ref, core), (other_ref, 1 - core)):
        begin = ((plane * 2 + holder) * nz + z) * per_device
        logits = product(rows_ref[...], every_ref[:, :D])
        picked = picked + jnp.sum(jnp.where(line == ids - begin, logits, 0.0), axis=0, keepdims=True)
        top = jnp.max(logits, axis=0, keepdims=True)
        tops.append(top)
        sums.append(jnp.sum(jnp.exp(logits - top), axis=0, keepdims=True))
    top = jnp.maximum(tops[0], tops[1])
    total = sums[0] * jnp.exp(tops[0] - top) + sums[1] * jnp.exp(tops[1] - top)
    entropy = top + jnp.log(total)
    for k in range(planes):
        for part, value in ((0, entropy), (1, picked)):
            pair_ref[k * nz : (k + 1) * nz, part * slot_dev : (part + 1) * slot_dev] = (
                jnp.broadcast_to(value[:, k * slot_dev : (k + 1) * slot_dev], (nz, slot_dev))
            )

    slot = lax.broadcasted_iota(jnp.int32, (1, slots), 1)
    flags = notes[1:2, :]
    counts = jnp.where(slot % slot_dev == 0, notes[2:3, :], 0.0)
    both = flags + counts
    total_ref[...] = jnp.sum(both, axis=1, keepdims=True).astype(jnp.int32)
    before = jnp.sum(jnp.where(slot // slot_dev < plane, both, 0.0), axis=1, keepdims=True)
    partner = jnp.sum(jnp.where(slot == plane * slot_dev, counts, 0.0), axis=1, keepdims=True)
    before = (before + jnp.where(core == 1, partner, 0.0)).astype(jnp.int32)
    freed = (flag_ref[...] == 1).astype(jnp.int32)
    below = lax.broadcasted_iota(jnp.int32, (slot_dev, slot_dev), 0)
    place = lax.broadcasted_iota(jnp.int32, (slot_dev, slot_dev), 1)
    ahead = jnp.sum(jnp.where(below < place, as_column(freed), 0), axis=0, keepdims=True)
    rank_ref[...] = jnp.where(freed == 1, ahead + before, -1)


def vocab_stats(every, own, other, flag, nz):
    slots = every.shape[0]
    rows = own.shape[0]
    slot_dev = flag.shape[1]
    return pl.pallas_call(
        vocab_kernel,
        in_specs=in_vmem(4),
        out_specs=in_vmem(3),
        out_shape=[
            jax.ShapeDtypeStruct((slots // slot_dev * nz, 2 * slot_dev), jnp.float32),
            jax.ShapeDtypeStruct((1, slot_dev), jnp.int32),
            jax.ShapeDtypeStruct((1, 1), jnp.int32),
        ],
        compiler_params=params(20),
        cost_estimate=pl.CostEstimate(
            flops=4 * rows * slots * D, bytes_accessed=4 * rows * D, transcendentals=2 * rows * slots
        ),
        name="vocab_stats",
    )(every, own, other, flag)


def on_device(
    query,
    incoming_key,
    new_value,
    key_cache,
    value_cache,
    cache_len,
    out_weight,
    residual,
    post_gain,
    final_gain,
    vocab_weight,
    sampled,
    stop_flag,
):
    slot_dev = query.shape[0]
    nz = lax.axis_size("tensor")
    planes = lax.axis_size(PLANE)
    other_flag = other_core(stop_flag)

    blocks = attend(
        query, incoming_key, new_value, key_cache, value_cache, cache_len, out_weight, nz
    )
    flag, sampled_line = stop_flag.reshape(1, slot_dev), sampled.reshape(1, slot_dev)
    blocks, vocab_weight, other_flag, flag, sampled_line = lax.optimization_barrier(
        (blocks, vocab_weight, other_flag, flag, sampled_line)
    )
    vocab_other = other_core(vocab_weight)
    pieces = exchange(blocks, "tensor")
    mix = exchange(mix_rows(pieces, residual, post_gain), "tensor")
    hidden, new_residual = hidden_blocks(
        mix,
        final_gain,
        sampled_line,
        flag,
        other_flag.reshape(1, slot_dev),
        planes,
    )
    every = exchange(hidden, PLANE).reshape(planes * slot_dev, D + META)
    pair, rank, released = vocab_stats(every, vocab_weight, vocab_other, flag, nz)
    gathered = exchange(pair, CHIPS)
    parts = gathered[:, :slot_dev]
    highest = jnp.max(parts, axis=0)
    overall = jnp.log(jnp.sum(jnp.exp(parts - highest[None]), axis=0)) + highest
    token_logprob = jnp.sum(gathered[:, slot_dev:], axis=0) - overall
    return (new_residual, token_logprob, rank.reshape(slot_dev), released.reshape(()))


def solution(mesh):
    split = Mesh(
        mesh.devices.reshape(4, 4, 2, mesh.shape["tensor"]), ("dp_0", "dp_1", "dp_2", "tensor")
    )
    in_specs = (
        P(DP, "tensor"),
        P(DP, "tensor"),
        P(DP, "tensor"),
        P(DP, None, "tensor"),
        P(DP, None, "tensor"),
        P(DP),
        P("tensor", None),
        P(DP, None),
        P(),
        P(),
        P(DP_TENSOR, None),
        P(DP),
        P(DP),
    )
    out_specs = (P(DP, "tensor"), P(DP), P(DP), P())
    return jax.shard_map(
        on_device, mesh=split, in_specs=in_specs, out_specs=out_specs, check_vma=False
    )
```
